32 devices in a mesh: gx: 4 (over y, core), gy: 2 (over x), gz: 4 (over z).
Axes of the slice: x: 2, y: 2, z: 4, core: 2. Of those that a mesh axis runs over, the one named last changes fastest.
Arguments:
- node_latent: bfloat16 [64, 64, 16, 128], P('gx', 'gy', 'gz'), may hold values from -6 to 6
- edge_latent: bfloat16 [4, 2, 4, 12288, 128], P('gx', 'gy', 'gz'), may hold values from -6 to 6
- senders: int32 [4, 2, 4, 12288], P('gx', 'gy', 'gz'), may hold values from 7 to 3664, as said below
- receivers: int32 [4, 2, 4, 12288], P('gx', 'gy', 'gz'), may hold values from 0 to 2047, as said below
- w1_edge: bfloat16 [384, 128], replicated, may hold values from -0.3125 to 0.3125
- b1_edge: float32 [128], replicated, may hold values from -3 to 3
- w2_edge: bfloat16 [128, 128], replicated, may hold values from -0.5 to 0.5
- b2_edge: float32 [128], replicated, may hold values from -3 to 3
- w1_node: bfloat16 [256, 128], replicated, may hold values from -0.375 to 0.375
- b1_node: float32 [128], replicated, may hold values from -3 to 3
- w2_node: bfloat16 [128, 128], replicated, may hold values from -0.5 to 0.5
- cot_node: bfloat16 [64, 64, 16, 128], P('gx', 'gy', 'gz'), may hold values from -6 to 6
- cot_edge: bfloat16 [4, 2, 4, 12288, 128], P('gx', 'gy', 'gz'), may hold values from -8 to 8
Outputs:
- grad_node: bfloat16 [64, 64, 16, 128], P('gx', 'gy', 'gz')
- grad_edge: bfloat16 [4, 2, 4, 12288, 128], P('gx', 'gy', 'gz')
- grad_w1_edge: float32 [384, 128], replicated
- grad_w2_edge: float32 [128, 128], replicated
- grad_w1_node: float32 [256, 128], replicated
- grad_w2_node: float32 [128, 128], replicated
- grad_biases: float32 [4, 128], replicated
The draws below stay inside these ranges and needn't reach their ends.
Inputs may be any that keep to these rules, and one draw needn't show every extreme that they name: `receivers`: in every block the list is nondecreasing; entry (i * 32 + j) * 4 + l names the block's cell at local coordinates (i, j, l). `senders`: entry (p * 34 + q) * 6 + r names the cell at local coordinates (p - 1, q - 1, r - 1) of the block extended by one cell on every side, the extension being cells of the adjacent blocks around the periodic box; it is always one of the six face neighbours of the same slot's receiver.
All inputs are finite; a program needn't handle non-finite values.
Results may differ from the reference program's by a relative error of at most 0.01.
Values may be sent and summed in bfloat16 or wider, within the bound.
A program may use at most 128 MiB of HBM per device.

```python
import jax
import jax.numpy as jnp
from jax import lax

H = 128
BX = 16
BY = 32
BZ = 4
CELLS = 2048
EDGES_DEV = 12288
NX = 64
NY = 64
NZ = 16
PARAMS = 115200
N_GX = 4
N_GY = 2
N_GZ = 4


def edge_lists(key):
    base_key = jax.random.fold_in(key, 7)
    receiver_key, direction_key = jax.random.split(base_key)
    grid_shape = (N_GX, N_GY, N_GZ, EDGES_DEV)
    receiver_ids = jnp.sort(jax.random.randint(receiver_key, grid_shape, 0, BX * BY * BZ), axis=-1)
    direction = jax.random.randint(direction_key, grid_shape, 0, 6)
    along_x = receiver_ids // (BY * BZ)
    along_y = receiver_ids // BZ % BY
    along_z = receiver_ids % BZ
    step_x = (direction == 0).astype(jnp.int32) - (direction == 1).astype(jnp.int32)
    step_y = (direction == 2).astype(jnp.int32) - (direction == 3).astype(jnp.int32)
    step_z = (direction == 4).astype(jnp.int32) - (direction == 5).astype(jnp.int32)
    sender_ids = ((along_x + 1 + step_x) * (BY + 2) + along_y + 1 + step_y) * (BZ + 2) + along_z + 1 + step_z
    return (sender_ids.astype(jnp.int32), receiver_ids.astype(jnp.int32))


def draw_senders(key, part):
    return edge_lists(key)[0]


def draw_receivers(key, part):
    return edge_lists(key)[1]


def draw_cot_edge(key, part):
    base_key = jax.random.fold_in(key, 23)
    noise_key, common_key, scale_key = jax.random.split(base_key, 3)
    grid_shape = (N_GX, N_GY, N_GZ, EDGES_DEV, H)
    noise_part = jax.random.normal(noise_key, grid_shape, jnp.float32)
    values = noise_part
    return jnp.clip(values, -8.0, 8.0).astype(jnp.bfloat16)


def steps_of(rng, dims, pieces, smallest, top_value):
    def one(dim, parts):
        heights = jax.random.uniform(jax.random.fold_in(jax.random.fold_in(rng, 6), dim), (parts,), jnp.float32, smallest / len(pieces), top_value / len(pieces))
        return jnp.repeat(jnp.exp(heights), dims[dim] // parts).reshape((-1,) + (1,) * (len(dims) - dim - 1))

    loudness = one(*pieces[0])
    for cut in pieces[1:]:
        loudness = loudness * one(*cut)
    return loudness


def bell_draw(stream_key, dims, spread, reach, cuts=(), kind=jnp.bfloat16):
    array = spread * jax.random.normal(stream_key, dims, jnp.float32)
    if cuts:
        array = array * steps_of(stream_key, dims, cuts, -0.22, 0.18)
    return jnp.clip(array, -reach, reach).astype(kind)


def setup_inputs(seed: int = 0) -> dict:
    seeds = jax.random.split(jax.random.key(seed), 14)
    node_latent = bell_draw(seeds[0], (NX, NY, NZ, H), 1.0, 6.0, ((0, 4), (1, 2), (2, 4)))
    edge_latent = bell_draw(seeds[1], (N_GX, N_GY, N_GZ, EDGES_DEV, H), 1.0, 6.0, ((0, 4), (1, 2), (2, 4)))
    senders = draw_senders(jax.random.fold_in(seeds[13], 71), 0)
    receivers = draw_receivers(jax.random.fold_in(seeds[13], 71), 0)
    w1_edge = bell_draw(seeds[4], (3 * H, H), (3 * H) ** -0.5, 0.3125)
    b1_edge = bell_draw(seeds[5], (H,), 0.5, 3.0, (), jnp.float32)
    w2_edge = bell_draw(seeds[6], (H, H), H ** -0.5, 0.5)
    b2_edge = bell_draw(seeds[7], (H,), 0.5, 3.0, (), jnp.float32)
    w1_node = bell_draw(seeds[8], (2 * H, H), (2 * H) ** -0.5, 0.375)
    b1_node = bell_draw(seeds[9], (H,), 0.5, 3.0, (), jnp.float32)
    w2_node = bell_draw(seeds[10], (H, H), H ** -0.5, 0.5)
    cot_node = bell_draw(seeds[11], (NX, NY, NZ, H), 1.0, 6.0, ((0, 4), (1, 2), (2, 4)))
    cot_edge = draw_cot_edge(jax.random.fold_in(seeds[13], 71), 0)
    return dict(node_latent=node_latent, edge_latent=edge_latent, senders=senders, receivers=receivers, w1_edge=w1_edge, b1_edge=b1_edge, w2_edge=w2_edge, b2_edge=b2_edge, w1_node=w1_node, b1_node=b1_node, w2_node=w2_node, cot_node=cot_node, cot_edge=cot_edge)


def column_sums(values):
    return lax.optimization_barrier(jnp.sum(values.astype(jnp.float32), axis=0))

def silu_slope(values):
    sigma = jax.nn.sigmoid(values)
    return sigma * (1.0 + values * (1.0 - sigma))

def block_terms(padded, edge_rows, cot_rows, cot_cells, sender_ids, receiver_ids, w1_edge, b1_edge, w2_edge, b2_edge, w1_node, b1_node, w2_node):
    latent = edge_rows.shape[1]
    cell_count = cot_cells.shape[0]
    flat_pad = padded.reshape(-1, latent)
    own_rows = padded[1:-1, 1:-1, 1:-1].reshape(cell_count, latent)
    sender_rows = jnp.take(flat_pad, sender_ids, axis=0)
    receiver_rows = jnp.take(own_rows, receiver_ids, axis=0)
    x_edge = jnp.concatenate([edge_rows, sender_rows, receiver_rows], axis=1)
    z_edge = jnp.dot(x_edge, w1_edge, preferred_element_type=jnp.float32) + b1_edge
    u_edge = jax.nn.silu(z_edge).astype(jnp.bfloat16)
    edge_new = (edge_rows.astype(jnp.float32) + jnp.dot(u_edge, w2_edge, preferred_element_type=jnp.float32) + b2_edge).astype(jnp.bfloat16)
    aggregate = jax.ops.segment_sum(edge_new.astype(jnp.float32), receiver_ids, cell_count, indices_are_sorted=True).astype(jnp.bfloat16)
    x_node = jnp.concatenate([own_rows, aggregate], axis=1)
    z_node = jnp.dot(x_node, w1_node, preferred_element_type=jnp.float32) + b1_node
    u_node = jax.nn.silu(z_node).astype(jnp.bfloat16)
    dz_node = (jnp.dot(cot_cells, w2_node.T, preferred_element_type=jnp.float32) * silu_slope(z_node)).astype(jnp.bfloat16)
    dx_node = jnp.dot(dz_node, w1_node.T, preferred_element_type=jnp.float32)
    d_edge = (cot_rows.astype(jnp.float32) + jnp.take(dx_node[:, latent:], receiver_ids, axis=0)).astype(jnp.bfloat16)
    dz_edge = (jnp.dot(d_edge, w2_edge.T, preferred_element_type=jnp.float32) * silu_slope(z_edge)).astype(jnp.bfloat16)
    dx_edge = jnp.dot(dz_edge, w1_edge.T, preferred_element_type=jnp.float32)
    grad_edge = (d_edge.astype(jnp.float32) + dx_edge[:, :latent]).astype(jnp.bfloat16)
    receiver_sum = jax.ops.segment_sum(dx_edge[:, 2 * latent:], receiver_ids, cell_count, indices_are_sorted=True)
    sender_sum = jax.ops.segment_sum(dx_edge[:, latent:2 * latent], sender_ids, flat_pad.shape[0])
    local_rows = dx_node[:, :latent] + receiver_sum
    raws = (jnp.dot(x_edge.T, dz_edge, preferred_element_type=jnp.float32), column_sums(dz_edge), jnp.dot(u_edge.T, d_edge, preferred_element_type=jnp.float32), column_sums(d_edge), jnp.dot(x_node.T, dz_node, preferred_element_type=jnp.float32), column_sums(dz_node), jnp.dot(u_node.T, cot_cells, preferred_element_type=jnp.float32), column_sums(cot_cells))
    return (grad_edge, local_rows, sender_sum, raws)

def reference(node_latent, edge_latent, senders, receivers, w1_edge, b1_edge, w2_edge, b2_edge, w1_node, b1_node, w2_node, cot_node, cot_edge):
    block_total = N_GX * N_GY * N_GZ
    halo_grid = jnp.pad(node_latent, ((1, 1), (1, 1), (1, 1), (0, 0)), mode='wrap')
    edge_blocks = edge_latent.reshape(block_total, EDGES_DEV, H)
    cot_blocks = cot_edge.reshape(block_total, EDGES_DEV, H)
    sender_blocks = senders.reshape(block_total, EDGES_DEV)
    receiver_blocks = receivers.reshape(block_total, EDGES_DEV)
    zero_index = jnp.zeros((), jnp.int32)
    shapes = ((3 * H, H), (H,), (H, H), (H,), (2 * H, H), (H,), (H, H), (H,))
    totals = tuple((jnp.zeros(shape_item, jnp.float32) for shape_item in shapes))
    grad_grid = jnp.zeros((NX + 2, NY + 2, NZ + 2, H), jnp.float32)

    def block_step(running, inputs):
        grid_now, totals_now = running
        block_index, edge_rows, cot_rows, sender_ids, receiver_ids = inputs
        corner_x = (block_index // (N_GY * N_GZ) * BX).astype(jnp.int32)
        corner_y = (block_index // N_GZ % N_GY * BY).astype(jnp.int32)
        corner_z = (block_index % N_GZ * BZ).astype(jnp.int32)
        anchor = (corner_x, corner_y, corner_z, zero_index)
        padded = lax.dynamic_slice(halo_grid, anchor, (BX + 2, BY + 2, BZ + 2, H))
        cot_cells = lax.dynamic_slice(cot_node, anchor, (BX, BY, BZ, H)).reshape(CELLS, H)
        grad_edge, local_rows, sender_sum, raws = block_terms(padded, edge_rows, cot_rows, cot_cells, sender_ids, receiver_ids, w1_edge, b1_edge, w2_edge, b2_edge, w1_node, b1_node, w2_node)
        block_grad = sender_sum.reshape(BX + 2, BY + 2, BZ + 2, H)
        block_grad = block_grad.at[1:-1, 1:-1, 1:-1].add(local_rows.reshape(BX, BY, BZ, H))
        current = lax.dynamic_slice(grid_now, anchor, (BX + 2, BY + 2, BZ + 2, H))
        grid_now = lax.dynamic_update_slice(grid_now, current + block_grad, anchor)
        totals_now = tuple((older + fresh for older, fresh in zip(totals_now, raws)))
        return ((grid_now, totals_now), grad_edge)
    block_ids = jnp.arange(block_total, dtype=jnp.int32)
    (grad_grid, totals), edge_grads = lax.scan(block_step, (grad_grid, totals), (block_ids, edge_blocks, cot_blocks, sender_blocks, receiver_blocks))
    folded = grad_grid.at[1].add(grad_grid[-1]).at[-2].add(grad_grid[0])
    folded = folded.at[:, 1].add(folded[:, -1]).at[:, -2].add(folded[:, 0])
    folded = folded.at[:, :, 1].add(folded[:, :, -1]).at[:, :, -2].add(folded[:, :, 0])
    grad_node = (cot_node.astype(jnp.float32) + folded[1:-1, 1:-1, 1:-1]).astype(jnp.bfloat16)
    grad_edge = edge_grads.reshape(N_GX, N_GY, N_GZ, EDGES_DEV, H)
    squares = sum((jnp.sum(entry * entry) for entry in totals))
    factor = 1.0 / jnp.maximum(1.0, jnp.sqrt(squares / PARAMS))
    grad_w1_edge = totals[0] * factor
    grad_w2_edge = totals[2] * factor
    grad_w1_node = totals[4] * factor
    grad_w2_node = totals[6] * factor
    grad_biases = jnp.stack([totals[1], totals[3], totals[5], totals[7]]) * factor
    return (grad_node, grad_edge, grad_w1_edge, grad_w2_edge, grad_w1_node, grad_w2_node, grad_biases)
```

```python
import functools

import jax
import jax.numpy as jnp
from jax import lax
from jax.experimental import pallas as pl
from jax.experimental.pallas import tpu as pltpu
from jax.sharding import PartitionSpec as P

F32 = jnp.float32
BF16 = jnp.bfloat16
TILE = 256
WIN = 80
WIDE = 128
ROUND = 16


def dot(left, right):
    return jnp.dot(left, right, preferred_element_type=F32)


def dot_t(left, right):
    return lax.dot_general(left, right, (((0,), (0,)), ((), ())), preferred_element_type=F32)


def dot_nt(left, right):
    return lax.dot_general(left, right, (((1,), (1,)), ((), ())), preferred_element_type=F32)


def sigma_of(values):
    return 0.5 + 0.5 * jnp.tanh(0.5 * values)


def fold_rows(values):
    return jnp.sum(values.reshape(-1, 8, values.shape[-1]), axis=0)


def layer_kernel(
    dims,
    stride,
    base_ref, count_ref,
    node_ref, edge_ref, cot_ref, cotn_ref, key_ref,
    w1e_ref, b1e_ref, w2e_ref, b2e_ref, w1n_ref, b1n_ref, w2n_ref,
    fxp_ref, fxm_ref, fyp_ref, fym_ref, fzp_ref, fzm_ref,
    gnode_ref, gedge_ref, raw_ref,
    oxp_ref, oxm_ref, oyp_ref, oym_ref, ozp_ref, ozm_ref,
    tab_ref, s_ref, r_ref, tmp_ref, z_ref, agg_ref, dagg_ref, bias_ref, rawr_ref, *g_refs,
):
    sx, sy, sz = dims
    cells = sx * sy * sz
    plane = sy * sz
    lat = node_ref.shape[1]
    tiles = edge_ref.shape[0] // TILE
    h = lat
    slab = 256
    slabs = cells // slab

    w1s = w1e_ref[h:2 * h, :]
    w1r = w1e_ref[2 * h:, :]

    for k in range(slabs):
        rows = pl.ds(k * slab, slab)
        s_ref[rows, :] = dot(node_ref[rows, :], w1s)
        r_ref[rows, :] = dot(node_ref[rows, :], w1r) + b1e_ref[...]

    def publish(d):
        for k in range(slabs):
            rows = pl.ds(k * slab, slab)
            tab_ref[d, rows, :] = (tmp_ref[rows, :] + r_ref[rows, :]).astype(BF16)
        tab_ref[d, pl.ds(cells, WIDE), :] = jnp.zeros((WIDE, h), BF16)

    def shift_up(by):
        for k in range(slabs):
            n = min(slab, cells - by - k * slab)
            if n > 0:
                tmp_ref[pl.ds(k * slab, n), :] = s_ref[pl.ds(k * slab + by, n), :]

    def shift_down(by):
        for k in range(slabs):
            n = min(slab, cells - by - k * slab)
            if n > 0:
                tmp_ref[pl.ds(k * slab + by, n), :] = s_ref[pl.ds(k * slab, n), :]

    shift_up(plane)
    tmp_ref[pl.ds(cells - plane, plane), :] = dot(fxp_ref[...], w1s)
    publish(0)
    shift_down(plane)
    tmp_ref[pl.ds(0, plane), :] = dot(fxm_ref[...], w1s)
    publish(1)
    shift_up(sz)
    face = dot(fyp_ref[...], w1s)
    for i in range(sx):
        tmp_ref[pl.ds(i * plane + plane - sz, sz), :] = face[i * sz:(i + 1) * sz]
    publish(2)
    shift_down(sz)
    face = dot(fym_ref[...], w1s)
    for i in range(sx):
        tmp_ref[pl.ds(i * plane, sz), :] = face[i * sz:(i + 1) * sz]
    publish(3)
    shift_up(1)
    tmp_ref[pl.ds(sz - 1, sx * sy, stride=sz), :] = dot(fzp_ref[...], w1s)
    publish(4)
    shift_down(1)
    tmp_ref[pl.ds(0, sx * sy, stride=sz), :] = dot(fzm_ref[...], w1s)
    publish(5)

    for k in range(slabs):
        rows = pl.ds(k * slab, slab)
        agg_ref[rows, :] = jnp.zeros((slab, h), F32)
        for g_ref in g_refs:
            g_ref[rows, :] = jnp.zeros((slab, h), F32)
    agg_ref[pl.ds(cells, WIDE), :] = jnp.zeros((WIDE, h), F32)
    dagg_ref[pl.ds(cells, WIDE), :] = jnp.zeros((WIDE, h), BF16)
    for g_ref in g_refs:
        g_ref[pl.ds(cells, WIDE), :] = jnp.zeros((WIDE, h), F32)
    rawr_ref[...] = jnp.zeros_like(rawr_ref)
    bias_ref[...] = jnp.zeros_like(bias_ref)

    lane_chunks = (6 * WIN + 127) // 128

    def lane_values():
        out = []
        for q in range(lane_chunks):
            m = lax.broadcasted_iota(jnp.int32, (1, 128), 1) + 128 * q
            d = jnp.zeros((1, 128), jnp.int32)
            for k in range(1, 6):
                d = d + (m >= k * WIN).astype(jnp.int32)
            out.append(jnp.where(m < 6 * WIN, m + d * (stride - WIN), -(1 << 30)))
        return out

    def columns(row):
        parts = [
            jnp.broadcast_to(row[:, q * 128:(q + 1) * 128], (128, 128)).T
            for q in range(TILE // 128)
        ]
        return jnp.concatenate(parts, axis=0)

    def hot_cols(col, b):
        col = col - b
        pieces = [jnp.where(col == v, 1.0, 0.0).astype(BF16) for v in lane_values()]
        return jnp.concatenate(pieces, axis=1)

    def gather_table(col, b):
        pieces = [tab_ref[d, pl.ds(b, WIN), :] for d in range(6)]
        pad = lane_chunks * 128 - 6 * WIN
        if pad:
            pieces.append(jnp.zeros((pad, h), BF16))
        return dot(hot_cols(col, b), jnp.concatenate(pieces, axis=0))

    def hot_cell_rows(row, b, width):
        cell = (row & (stride - 1)) - b
        return jnp.where(
            lax.broadcasted_iota(jnp.int32, (width, TILE), 0) == cell, 1.0, 0.0
        ).astype(BF16)

    def hot_cell_cols(col, b, width):
        cell = (col & (stride - 1)) - b
        return jnp.where(
            lax.broadcasted_iota(jnp.int32, (TILE, width), 1) == cell, 1.0, 0.0
        ).astype(BF16)

    def hot_dir_rows(row, b):
        iota = lax.broadcasted_iota(jnp.int32, (WIN, TILE), 0)
        pieces = [
            jnp.where(iota == row - (b + d * stride), 1.0, 0.0).astype(BF16) for d in range(6)
        ]
        return jnp.concatenate(pieces, axis=0)

    w1a = w1e_ref[:h, :]

    def forward_tile(t, slow):
        rows = pl.ds(pl.multiple_of(t * TILE, TILE), TILE)
        b = pl.multiple_of(base_ref[t], ROUND)
        row = key_ref[pl.ds(t, 1), :]
        col = columns(row)
        e = edge_ref[rows, :]
        z = dot(e, w1a) + gather_table(col, b)
        z_ref[rows, :] = z
        if slow:
            @pl.loop(1, count_ref[t])
            def _(w):
                z_ref[rows, :] += gather_table(col, pl.multiple_of(b + w * WIN, ROUND))
            z = z_ref[rows, :]
        u = (z * sigma_of(z)).astype(BF16)
        fresh = (e.astype(F32) + dot(u, w2e_ref[...]) + b2e_ref[...]).astype(BF16)

        def scatter(at):
            agg_ref[pl.ds(at, WIN), :] += dot(hot_cell_rows(row, at, WIN), fresh)

        scatter(b)
        if slow:
            @pl.loop(1, count_ref[t])
            def _(w):
                scatter(pl.multiple_of(b + w * WIN, ROUND))

    def backward_tile(t, slow):
        rows = pl.ds(pl.multiple_of(t * TILE, TILE), TILE)
        b = pl.multiple_of(base_ref[t], ROUND)
        row = key_ref[pl.ds(t, 1), :]
        col = columns(row)

        def gather(at):
            hot = hot_cell_cols(col, at, WIDE)
            if slow:
                keep = lax.broadcasted_iota(jnp.int32, (1, WIDE), 1) < WIN
                hot = jnp.where(keep, hot.astype(F32), 0.0).astype(BF16)
            return dot(hot, dagg_ref[pl.ds(at, WIDE), :])

        back = gather(b)
        if slow:
            def more(w, back):
                return back + gather(pl.multiple_of(b + w * WIN, ROUND))
            back = lax.fori_loop(1, count_ref[t], more, back)
        e = edge_ref[rows, :]
        d = (cot_ref[rows, :].astype(F32) + back).astype(BF16)
        z = z_ref[rows, :]
        s = sigma_of(z)
        u = z * s
        slope = s * (1.0 + z * (1.0 - s))
        dz = dot_nt(d, w2e_ref[...]) * slope
        dzb = dz.astype(BF16)
        gedge_ref[rows, :] = (d.astype(F32) + dot_nt(dzb, w1a)).astype(BF16)

        def scatter(at):
            out = dot(hot_dir_rows(row, at), dzb)
            for k, g_ref in enumerate(g_refs):
                g_ref[pl.ds(at, WIN), :] += out[k * WIN:(k + 1) * WIN]

        scatter(b)
        if slow:
            @pl.loop(1, count_ref[t])
            def _(w):
                scatter(pl.multiple_of(b + w * WIN, ROUND))
        raw_ref[0:h, :] += dot_t(e, dzb)
        raw_ref[3 * h:4 * h, :] += dot_t(u.astype(BF16), d)
        bias_ref[0] += fold_rows(dzb.astype(F32))
        bias_ref[1] += fold_rows(d.astype(F32))

    raw_ref[...] = jnp.zeros_like(raw_ref)
    most = lax.fori_loop(0, tiles, lambda t, m: jnp.maximum(m, count_ref[t]), 1)

    @pl.when(most == 1)
    def _():
        @pl.loop(0, tiles)
        def _(t):
            forward_tile(t, False)

    @pl.when(most > 1)
    def _():
        @pl.loop(0, tiles)
        def _(t):
            forward_tile(t, True)

    at = 4 * h

    @pl.loop(0, slabs)
    def _(k):
        rows = pl.ds(pl.multiple_of(k * slab, slab), slab)
        own = node_ref[rows, :]
        agg = agg_ref[rows, :].astype(BF16)
        cot = cotn_ref[rows, :]
        z = dot(own, w1n_ref[:h, :]) + dot(agg, w1n_ref[h:, :]) + b1n_ref[...]
        s = sigma_of(z)
        u = (z * s).astype(BF16)
        dz = (dot_nt(cot, w2n_ref[...]) * (s * (1.0 + z * (1.0 - s)))).astype(BF16)
        gnode_ref[rows, :] = cot.astype(F32) + dot_nt(dz, w1n_ref[:h, :])
        dagg_ref[rows, :] = dot_nt(dz, w1n_ref[h:, :]).astype(BF16)
        raw_ref[at:at + h, :] += dot_t(own, dz)
        raw_ref[at + h:at + 2 * h, :] += dot_t(agg, dz)
        raw_ref[at + 2 * h:at + 3 * h, :] += dot_t(u, cot)
        bias_ref[2] += fold_rows(dz.astype(F32))
        bias_ref[3] += fold_rows(cot.astype(F32))

    @pl.when(most == 1)
    def _():
        @pl.loop(0, tiles)
        def _(t):
            backward_tile(t, False)

    @pl.when(most > 1)
    def _():
        @pl.loop(0, tiles)
        def _(t):
            backward_tile(t, True)

    g0, g1, g2, g3, g4, g5 = g_refs
    for k in range(slabs):
        rows = pl.ds(k * slab, slab)
        total = g0[rows, :] + g1[rows, :] + g2[rows, :] + g3[rows, :] + g4[rows, :] + g5[rows, :]
        total = total.astype(BF16)
        gnode_ref[rows, :] += dot_nt(total, w1r)
        rawr_ref[...] += dot_t(node_ref[rows, :], total)
    raw_ref[2 * h:3 * h, :] = rawr_ref[...]

    acc = jnp.zeros((h, h), F32)

    def out_face(values, own_ref, out_ref):
        values = values.astype(BF16)
        out_ref[...] = dot_nt(values, w1s).astype(BF16)
        return dot_t(own_ref[...], values)

    acc += out_face(g0[pl.ds(cells - plane, plane), :], fxp_ref, oxp_ref)
    acc += out_face(g1[pl.ds(0, plane), :], fxm_ref, oxm_ref)
    pieces = [g2[pl.ds(i * plane + plane - sz, sz), :] for i in range(sx)]
    acc += out_face(jnp.concatenate(pieces, axis=0), fyp_ref, oyp_ref)
    pieces = [g3[pl.ds(i * plane, sz), :] for i in range(sx)]
    acc += out_face(jnp.concatenate(pieces, axis=0), fym_ref, oym_ref)
    acc += out_face(g4[pl.ds(sz - 1, sx * sy, stride=sz), :], fzp_ref, ozp_ref)
    acc += out_face(g5[pl.ds(0, sx * sy, stride=sz), :], fzm_ref, ozm_ref)
    for i in range(sx):
        g2[pl.ds(i * plane + plane - sz, sz), :] = jnp.zeros((sz, h), F32)
        g3[pl.ds(i * plane, sz), :] = jnp.zeros((sz, h), F32)
    g4[pl.ds(sz - 1, sx * sy, stride=sz), :] = jnp.zeros((sx * sy, h), F32)
    g5[pl.ds(0, sx * sy, stride=sz), :] = jnp.zeros((sx * sy, h), F32)

    tmp_ref[...] = jnp.zeros_like(tmp_ref)
    for g_ref, by in ((g0, plane), (g2, sz), (g4, 1)):
        for k in range(slabs):
            n = min(slab, cells - by - k * slab)
            if n > 0:
                tmp_ref[pl.ds(k * slab + by, n), :] += g_ref[pl.ds(k * slab, n), :]
    for g_ref, by in ((g1, plane), (g3, sz), (g5, 1)):
        for k in range(slabs):
            n = min(slab, cells - by - k * slab)
            if n > 0:
                tmp_ref[pl.ds(k * slab, n), :] += g_ref[pl.ds(k * slab + by, n), :]
    rawr_ref[...] = acc
    for k in range(slabs):
        rows = pl.ds(k * slab, slab)
        total = tmp_ref[rows, :].astype(BF16)
        gnode_ref[rows, :] += dot_nt(total, w1s)
        rawr_ref[...] += dot_t(node_ref[rows, :], total)
    raw_ref[h:2 * h, :] = rawr_ref[...]
    for k in range(4):
        raw_ref[7 * h + k:7 * h + k + 1, :] = jnp.sum(bias_ref[k], axis=0, keepdims=True)


def exchange(head, tail, axis):
    count = lax.axis_size(axis)
    up = [(i, (i + 1) % count) for i in range(count)]
    down = [((i + 1) % count, i) for i in range(count)]
    return lax.ppermute(head, axis, down), lax.ppermute(tail, axis, up)


def on_device(
    node_latent, edge_latent, senders, receivers,
    w1_edge, b1_edge, w2_edge, b2_edge, w1_node, b1_node, w2_node,
    cot_node, cot_edge,
):
    sx, sy, sz, lat = node_latent.shape
    cells = sx * sy * sz
    edges = edge_latent.shape[3]
    own = node_latent.reshape(cells, lat)
    faces = []
    faces += exchange(node_latent[0].reshape(-1, lat), node_latent[-1].reshape(-1, lat), "gx")
    faces += exchange(node_latent[:, 0].reshape(-1, lat), node_latent[:, -1].reshape(-1, lat), "gy")
    faces += exchange(
        node_latent[:, :, 0].reshape(-1, lat), node_latent[:, :, -1].reshape(-1, lat), "gz"
    )
    r = receivers.reshape(edges)
    s = senders.reshape(edges)
    padded = ((r // (sy * sz) + 1) * (sy + 2) + r // sz % sy + 1) * (sz + 2) + r % sz + 1
    diff = s - padded
    step_x = (sy + 2) * (sz + 2)
    step_y = sz + 2
    direction = jnp.where(
        diff == step_x, 0,
        jnp.where(
            diff == -step_x, 1,
            jnp.where(
                diff == step_y, 2, jnp.where(diff == -step_y, 3, jnp.where(diff == 1, 4, 5))
            ),
        ),
    )
    stride = 1
    while stride < cells + WIDE:
        stride *= 2
    tiles = edges // TILE
    keys = (direction * stride + r).reshape(tiles, TILE)
    grouped = r.reshape(tiles, TILE)
    base = grouped[:, 0] // ROUND * ROUND
    counts = (grouped[:, -1] - base) // WIN + 1

    face_rows = [f.shape[0] for f in faces]
    raw_rows = 7 * lat + 8
    vmem = pl.BlockSpec(memory_space=pltpu.VMEM)
    smem = pl.BlockSpec(memory_space=pltpu.SMEM)
    outs = pl.pallas_call(
        functools.partial(layer_kernel, (sx, sy, sz), stride),
        out_shape=[
            jax.ShapeDtypeStruct((cells, lat), F32),
            jax.ShapeDtypeStruct((edges, lat), BF16),
            jax.ShapeDtypeStruct((raw_rows, lat), F32),
        ] + [jax.ShapeDtypeStruct((n, lat), BF16) for n in face_rows],
        in_specs=[smem] * 2 + [vmem] * 18,
        out_specs=[vmem] * 9,
        scratch_shapes=[
            pltpu.VMEM((6, cells + WIDE, lat), BF16),
            pltpu.VMEM((cells, lat), F32),
            pltpu.VMEM((cells, lat), F32),
            pltpu.VMEM((cells, lat), F32),
            pltpu.VMEM((edges, lat), F32),
            pltpu.VMEM((cells + WIDE, lat), F32),
            pltpu.VMEM((cells + WIDE, lat), BF16),
            pltpu.VMEM((4, 8, lat), F32),
            pltpu.VMEM((lat, lat), F32),
        ] + [pltpu.VMEM((cells + WIDE, lat), F32)] * 6,
        compiler_params=pltpu.CompilerParams(vmem_limit_bytes=60 * 1024 * 1024),
        cost_estimate=pl.CostEstimate(
            flops=40 * edges * lat * lat, bytes_accessed=6 * edges * lat, transcendentals=0
        ),
    )(
        base, counts,
        own, edge_latent.reshape(edges, lat), cot_edge.reshape(edges, lat),
        cot_node.reshape(cells, lat), keys,
        w1_edge, b1_edge.reshape(1, lat), w2_edge, b2_edge.reshape(1, lat),
        w1_node, b1_node.reshape(1, lat), w2_node,
        *faces,
    )
    gnode, gedge, raw = outs[:3]
    oxp, oxm, oyp, oym, ozp, ozm = outs[3:]
    xm, xp = exchange(oxm, oxp, "gx")
    ym, yp = exchange(oym, oyp, "gy")
    zm, zp = exchange(ozm, ozp, "gz")
    grid = gnode.reshape(sx, sy, sz, lat)
    grid = grid.at[0].add(xp.reshape(sy, sz, lat).astype(F32))
    grid = grid.at[-1].add(xm.reshape(sy, sz, lat).astype(F32))
    grid = grid.at[:, 0].add(yp.reshape(sx, sz, lat).astype(F32))
    grid = grid.at[:, -1].add(ym.reshape(sx, sz, lat).astype(F32))
    grid = grid.at[:, :, 0].add(zp.reshape(sx, sy, lat).astype(F32))
    grid = grid.at[:, :, -1].add(zm.reshape(sx, sy, lat).astype(F32))
    grad_node = grid.astype(BF16)

    summed = lax.psum(raw, ("gx", "gy", "gz"))
    params = 7 * lat * lat + 4 * lat
    squares = jnp.sum(summed * summed)
    factor = 1.0 / jnp.maximum(1.0, jnp.sqrt(squares / params))
    scaled = summed * factor
    return (
        grad_node,
        gedge.reshape(edge_latent.shape),
        scaled[:3 * lat],
        scaled[3 * lat:4 * lat],
        scaled[4 * lat:6 * lat],
        scaled[6 * lat:7 * lat],
        scaled[7 * lat:7 * lat + 4],
    )


def solution(mesh):
    cell = P("gx", "gy", "gz", None)
    edge = P("gx", "gy", "gz", None, None)
    return jax.shard_map(
        on_device,
        mesh=mesh,
        in_specs=(cell, edge, cell, cell, P(), P(), P(), P(), P(), P(), P(), cell, edge),
        out_specs=(cell, edge, P(), P(), P(), P(), P()),
        check_vma=False,
    )
```

```python
import functools

import jax
import jax.numpy as jnp
from jax import lax
from jax.experimental import pallas as pl
from jax.experimental.pallas import tpu as pltpu
from jax.sharding import PartitionSpec as P

F32 = jnp.float32
BF16 = jnp.bfloat16
TILE = 256
WIN = 80
WIDE = 128
ROUND = 16


def dot(left, right):
    return jnp.dot(left, right, preferred_element_type=F32)


def dot_t(left, right):
    return lax.dot_general(left, right, (((0,), (0,)), ((), ())), preferred_element_type=F32)


def dot_nt(left, right):
    return lax.dot_general(left, right, (((1,), (1,)), ((), ())), preferred_element_type=F32)


def sigma_of(values):
    return 0.5 + 0.5 * jnp.tanh(0.5 * values)


def fold_rows(values):
    return jnp.sum(values.reshape(-1, 8, values.shape[-1]), axis=0)


def layer_kernel(
    dims,
    stride,
    base_ref, count_ref,
    node_ref, edge_ref, cot_ref, cotn_ref, key_ref,
    w1e_ref, b1e_ref, w2e_ref, b2e_ref, w1n_ref, b1n_ref, w2n_ref,
    fxp_ref, fxm_ref, fyp_ref, fym_ref, fzp_ref, fzm_ref,
    gnode_ref, gedge_ref, rawb_ref,
    oxp_ref, oxm_ref, oyp_ref, oym_ref, ozp_ref, ozm_ref,
    tab_ref, s_ref, r_ref, tmp_ref, z_ref, agg_ref, dagg_ref, bias_ref, rawr_ref, raw_ref, *g_refs,
):
    sx, sy, sz = dims
    cells = sx * sy * sz
    plane = sy * sz
    lat = node_ref.shape[1]
    tiles = edge_ref.shape[0] // TILE
    h = lat
    slab = 256
    slabs = cells // slab

    w1s = w1e_ref[h:2 * h, :]
    w1r = w1e_ref[2 * h:, :]

    for k in range(slabs):
        rows = pl.ds(k * slab, slab)
        s_ref[rows, :] = dot(node_ref[rows, :], w1s)
        r_ref[rows, :] = dot(node_ref[rows, :], w1r) + b1e_ref[...]

    def publish(d):
        for k in range(slabs):
            rows = pl.ds(k * slab, slab)
            tab_ref[d, rows, :] = (tmp_ref[rows, :] + r_ref[rows, :]).astype(BF16)
        tab_ref[d, pl.ds(cells, WIDE), :] = jnp.zeros((WIDE, h), BF16)

    def shift_up(by):
        for k in range(slabs):
            n = min(slab, cells - by - k * slab)
            if n > 0:
                tmp_ref[pl.ds(k * slab, n), :] = s_ref[pl.ds(k * slab + by, n), :]

    def shift_down(by):
        for k in range(slabs):
            n = min(slab, cells - by - k * slab)
            if n > 0:
                tmp_ref[pl.ds(k * slab + by, n), :] = s_ref[pl.ds(k * slab, n), :]

    shift_up(plane)
    tmp_ref[pl.ds(cells - plane, plane), :] = dot(fxp_ref[...], w1s)
    publish(0)
    shift_down(plane)
    tmp_ref[pl.ds(0, plane), :] = dot(fxm_ref[...], w1s)
    publish(1)
    shift_up(sz)
    face = dot(fyp_ref[...], w1s)
    for i in range(sx):
        tmp_ref[pl.ds(i * plane + plane - sz, sz), :] = face[i * sz:(i + 1) * sz]
    publish(2)
    shift_down(sz)
    face = dot(fym_ref[...], w1s)
    for i in range(sx):
        tmp_ref[pl.ds(i * plane, sz), :] = face[i * sz:(i + 1) * sz]
    publish(3)
    shift_up(1)
    tmp_ref[pl.ds(sz - 1, sx * sy, stride=sz), :] = dot(fzp_ref[...], w1s)
    publish(4)
    shift_down(1)
    tmp_ref[pl.ds(0, sx * sy, stride=sz), :] = dot(fzm_ref[...], w1s)
    publish(5)

    for k in range(slabs):
        rows = pl.ds(k * slab, slab)
        agg_ref[rows, :] = jnp.zeros((slab, h), F32)
        for g_ref in g_refs:
            g_ref[rows, :] = jnp.zeros((slab, h), F32)
    agg_ref[pl.ds(cells, WIDE), :] = jnp.zeros((WIDE, h), F32)
    dagg_ref[pl.ds(cells, WIDE), :] = jnp.zeros((WIDE, h), BF16)
    for g_ref in g_refs:
        g_ref[pl.ds(cells, WIDE), :] = jnp.zeros((WIDE, h), F32)
    rawr_ref[...] = jnp.zeros_like(rawr_ref)
    bias_ref[...] = jnp.zeros_like(bias_ref)

    lane_chunks = (6 * WIN + 127) // 128

    def lane_values():
        out = []
        for q in range(lane_chunks):
            m = lax.broadcasted_iota(jnp.int32, (1, 128), 1) + 128 * q
            d = jnp.zeros((1, 128), jnp.int32)
            for k in range(1, 6):
                d = d + (m >= k * WIN).astype(jnp.int32)
            out.append(jnp.where(m < 6 * WIN, m + d * (stride - WIN), -(1 << 30)))
        return out

    def columns(row):
        parts = [
            jnp.broadcast_to(row[:, q * 128:(q + 1) * 128], (128, 128)).T
            for q in range(TILE // 128)
        ]
        return jnp.concatenate(parts, axis=0)

    def hot_cols(col, b):
        col = col - b
        pieces = [jnp.where(col == v, 1.0, 0.0).astype(BF16) for v in lane_values()]
        return jnp.concatenate(pieces, axis=1)

    def gather_table(col, b):
        pieces = [tab_ref[d, pl.ds(b, WIN), :] for d in range(6)]
        pad = lane_chunks * 128 - 6 * WIN
        if pad:
            pieces.append(jnp.zeros((pad, h), BF16))
        return dot(hot_cols(col, b), jnp.concatenate(pieces, axis=0))

    def hot_cell_rows(row, b, width):
        cell = (row & (stride - 1)) - b
        return jnp.where(
            lax.broadcasted_iota(jnp.int32, (width, TILE), 0) == cell, 1.0, 0.0
        ).astype(BF16)

    def hot_cell_cols(col, b, width):
        cell = (col & (stride - 1)) - b
        return jnp.where(
            lax.broadcasted_iota(jnp.int32, (TILE, width), 1) == cell, 1.0, 0.0
        ).astype(BF16)

    def hot_dir_rows(row, b):
        iota = lax.broadcasted_iota(jnp.int32, (WIN, TILE), 0)
        pieces = [
            jnp.where(iota == row - (b + d * stride), 1.0, 0.0).astype(BF16) for d in range(6)
        ]
        return jnp.concatenate(pieces, axis=0)

    w1a = w1e_ref[:h, :]

    def forward_tile(t, slow):
        rows = pl.ds(pl.multiple_of(t * TILE, TILE), TILE)
        b = pl.multiple_of(base_ref[t], ROUND)
        row = key_ref[pl.ds(t, 1), :]
        col = columns(row)
        e = edge_ref[rows, :]
        z = dot(e, w1a) + gather_table(col, b)
        z_ref[rows, :] = z
        if slow:
            @pl.loop(1, count_ref[t])
            def _(w):
                z_ref[rows, :] += gather_table(col, pl.multiple_of(b + w * WIN, ROUND))
            z = z_ref[rows, :]
        u = (z * sigma_of(z)).astype(BF16)
        fresh = (e.astype(F32) + dot(u, w2e_ref[...]) + b2e_ref[...]).astype(BF16)

        def scatter(at):
            agg_ref[pl.ds(at, WIN), :] += dot(hot_cell_rows(row, at, WIN), fresh)

        scatter(b)
        if slow:
            @pl.loop(1, count_ref[t])
            def _(w):
                scatter(pl.multiple_of(b + w * WIN, ROUND))

    def backward_tile(t, slow):
        rows = pl.ds(pl.multiple_of(t * TILE, TILE), TILE)
        b = pl.multiple_of(base_ref[t], ROUND)
        row = key_ref[pl.ds(t, 1), :]
        col = columns(row)

        def gather(at):
            hot = hot_cell_cols(col, at, WIDE)
            if slow:
                keep = lax.broadcasted_iota(jnp.int32, (1, WIDE), 1) < WIN
                hot = jnp.where(keep, hot.astype(F32), 0.0).astype(BF16)
            return dot(hot, dagg_ref[pl.ds(at, WIDE), :])

        back = gather(b)
        if slow:
            def more(w, back):
                return back + gather(pl.multiple_of(b + w * WIN, ROUND))
            back = lax.fori_loop(1, count_ref[t], more, back)
        e = edge_ref[rows, :]
        d = (cot_ref[rows, :].astype(F32) + back).astype(BF16)
        z = z_ref[rows, :]
        s = sigma_of(z)
        u = z * s
        slope = s * (1.0 + z * (1.0 - s))
        dz = dot_nt(d, w2e_ref[...]) * slope
        dzb = dz.astype(BF16)
        gedge_ref[rows, :] = (d.astype(F32) + dot_nt(dzb, w1a)).astype(BF16)

        def scatter(at):
            out = dot(hot_dir_rows(row, at), dzb)
            for k, g_ref in enumerate(g_refs):
                g_ref[pl.ds(at, WIN), :] += out[k * WIN:(k + 1) * WIN]

        scatter(b)
        if slow:
            @pl.loop(1, count_ref[t])
            def _(w):
                scatter(pl.multiple_of(b + w * WIN, ROUND))
        raw_ref[0:h, :] += dot_t(e, dzb)
        raw_ref[3 * h:4 * h, :] += dot_t(u.astype(BF16), d)
        bias_ref[0] += fold_rows(dzb.astype(F32))
        bias_ref[1] += fold_rows(d.astype(F32))

    raw_ref[...] = jnp.zeros_like(raw_ref)
    most = lax.fori_loop(0, tiles, lambda t, m: jnp.maximum(m, count_ref[t]), 1)

    @pl.when(most == 1)
    def _():
        @pl.loop(0, tiles)
        def _(t):
            forward_tile(t, False)

    @pl.when(most > 1)
    def _():
        @pl.loop(0, tiles)
        def _(t):
            forward_tile(t, True)

    at = 4 * h

    @pl.loop(0, slabs)
    def _(k):
        rows = pl.ds(pl.multiple_of(k * slab, slab), slab)
        own = node_ref[rows, :]
        agg = agg_ref[rows, :].astype(BF16)
        cot = cotn_ref[rows, :]
        z = dot(own, w1n_ref[:h, :]) + dot(agg, w1n_ref[h:, :]) + b1n_ref[...]
        s = sigma_of(z)
        u = (z * s).astype(BF16)
        dz = (dot_nt(cot, w2n_ref[...]) * (s * (1.0 + z * (1.0 - s)))).astype(BF16)
        gnode_ref[rows, :] = cot.astype(F32) + dot_nt(dz, w1n_ref[:h, :])
        dagg_ref[rows, :] = dot_nt(dz, w1n_ref[h:, :]).astype(BF16)
        raw_ref[at:at + h, :] += dot_t(own, dz)
        raw_ref[at + h:at + 2 * h, :] += dot_t(agg, dz)
        raw_ref[at + 2 * h:at + 3 * h, :] += dot_t(u, cot)
        bias_ref[2] += fold_rows(dz.astype(F32))
        bias_ref[3] += fold_rows(cot.astype(F32))

    @pl.when(most == 1)
    def _():
        @pl.loop(0, tiles)
        def _(t):
            backward_tile(t, False)

    @pl.when(most > 1)
    def _():
        @pl.loop(0, tiles)
        def _(t):
            backward_tile(t, True)

    g0, g1, g2, g3, g4, g5 = g_refs
    for k in range(slabs):
        rows = pl.ds(k * slab, slab)
        total = g0[rows, :] + g1[rows, :] + g2[rows, :] + g3[rows, :] + g4[rows, :] + g5[rows, :]
        total = total.astype(BF16)
        gnode_ref[rows, :] += dot_nt(total, w1r)
        rawr_ref[...] += dot_t(node_ref[rows, :], total)
    raw_ref[2 * h:3 * h, :] = rawr_ref[...]

    acc = jnp.zeros((h, h), F32)

    def out_face(values, own_ref, out_ref):
        values = values.astype(BF16)
        out_ref[...] = dot_nt(values, w1s).astype(BF16)
        return dot_t(own_ref[...], values)

    acc += out_face(g0[pl.ds(cells - plane, plane), :], fxp_ref, oxp_ref)
    acc += out_face(g1[pl.ds(0, plane), :], fxm_ref, oxm_ref)
    pieces = [g2[pl.ds(i * plane + plane - sz, sz), :] for i in range(sx)]
    acc += out_face(jnp.concatenate(pieces, axis=0), fyp_ref, oyp_ref)
    pieces = [g3[pl.ds(i * plane, sz), :] for i in range(sx)]
    acc += out_face(jnp.concatenate(pieces, axis=0), fym_ref, oym_ref)
    acc += out_face(g4[pl.ds(sz - 1, sx * sy, stride=sz), :], fzp_ref, ozp_ref)
    acc += out_face(g5[pl.ds(0, sx * sy, stride=sz), :], fzm_ref, ozm_ref)
    for i in range(sx):
        g2[pl.ds(i * plane + plane - sz, sz), :] = jnp.zeros((sz, h), F32)
        g3[pl.ds(i * plane, sz), :] = jnp.zeros((sz, h), F32)
    g4[pl.ds(sz - 1, sx * sy, stride=sz), :] = jnp.zeros((sx * sy, h), F32)
    g5[pl.ds(0, sx * sy, stride=sz), :] = jnp.zeros((sx * sy, h), F32)

    tmp_ref[...] = jnp.zeros_like(tmp_ref)
    for g_ref, by in ((g0, plane), (g2, sz), (g4, 1)):
        for k in range(slabs):
            n = min(slab, cells - by - k * slab)
            if n > 0:
                tmp_ref[pl.ds(k * slab + by, n), :] += g_ref[pl.ds(k * slab, n), :]
    for g_ref, by in ((g1, plane), (g3, sz), (g5, 1)):
        for k in range(slabs):
            n = min(slab, cells - by - k * slab)
            if n > 0:
                tmp_ref[pl.ds(k * slab, n), :] += g_ref[pl.ds(k * slab + by, n), :]
    rawr_ref[...] = acc
    for k in range(slabs):
        rows = pl.ds(k * slab, slab)
        total = tmp_ref[rows, :].astype(BF16)
        gnode_ref[rows, :] += dot_nt(total, w1s)
        rawr_ref[...] += dot_t(node_ref[rows, :], total)
    raw_ref[h:2 * h, :] = rawr_ref[...]
    for k in range(4):
        raw_ref[7 * h + k:7 * h + k + 1, :] = jnp.sum(bias_ref[k], axis=0, keepdims=True)
    rawb_ref[...] = raw_ref[...].astype(BF16)


MESH = pl.DeviceIdType.MESH
AXES = ("gx", "gy", "gz")


def neighbours():
    here = [lax.axis_index(a) for a in AXES]
    out = []
    for k, a in enumerate(AXES):
        count = lax.axis_size(a)
        for step in (1, count - 1):
            at = list(here)
            at[k] = lax.rem(here[k] + step, count)
            out.append(tuple(at))
    return out


def halo_kernel(dims, node_ref, *refs):
    outs, sends, lands, tmp_ref, send_sem, recv_sem = (
        refs[:6], refs[6:12], refs[12:18], refs[18], refs[19], refs[20]
    )
    sx, sy, sz = dims
    plane = sy * sz
    cells = sx * plane
    ids = neighbours()
    barrier = pltpu.get_barrier_semaphore()
    for who in ids:
        pl.semaphore_signal(barrier, inc=1, device_id=who, device_id_type=MESH)
    for k in range(cells // 256):
        rows = pl.ds(k * 256, 256)
        tmp_ref[rows, :] = node_ref[rows, :].astype(F32)
    sends[4][...] = tmp_ref[pl.ds(sz - 1, sx * sy, stride=sz), :].astype(BF16)
    sends[5][...] = tmp_ref[pl.ds(0, sx * sy, stride=sz), :].astype(BF16)
    sends[0][...] = node_ref[pl.ds(cells - plane, plane), :]
    sends[1][...] = node_ref[pl.ds(0, plane), :]
    sends[2][...] = jnp.concatenate(
        [tmp_ref[pl.ds(i * plane + plane - sz, sz), :] for i in range(sx)], axis=0
    ).astype(BF16)
    sends[3][...] = jnp.concatenate(
        [tmp_ref[pl.ds(i * plane, sz), :] for i in range(sx)], axis=0
    ).astype(BF16)
    pl.semaphore_wait(barrier, 6)
    copies = []
    for d in (4, 5, 0, 1, 2, 3):
        copy = pltpu.make_async_remote_copy(
            src_ref=sends[d], dst_ref=lands[d ^ 1],
            send_sem=send_sem.at[d], recv_sem=recv_sem.at[d ^ 1],
            device_id=ids[d], device_id_type=MESH,
        )
        copy.start()
        copies.append((d, copy))
    for d, copy in copies:
        copy.wait_send()
    for d, copy in copies:
        copy.wait_recv()
        outs[d ^ 1][...] = lands[d ^ 1][...]


def reduce_kernel(dims, raw_ref, gnode_ref, *refs):
    faces = refs[:6]
    gout_ref, w1e_ref, w2e_ref, w1n_ref, w2n_ref, bias_ref = refs[6:12]
    part_ref, sum_ref, all_ref, tmp_ref = refs[12:16]
    lands = refs[16:22]
    rs_send, rs_recv, ag_send, ag_recv, halo_send, halo_recv = refs[22:28]
    sx, sy, sz = dims
    plane = sy * sz
    cells = sx * plane
    h = gnode_ref.shape[1]
    nx, ny, nz = [lax.axis_size(a) for a in AXES]
    n = nx * ny * nz
    ix, iy, iz = [lax.axis_index(a) for a in AXES]
    me = (ix * ny + iy) * nz + iz

    def rank(k):
        return lax.rem(me + k, n)

    def device(p):
        return (p // (ny * nz), p // nz % ny, p % nz)

    barrier = pltpu.get_barrier_semaphore()

    @pl.loop(1, n)
    def _(k):
        pl.semaphore_signal(barrier, inc=1, device_id=device(rank(k)), device_id_type=MESH)

    for k in range(cells // 256):
        rows = pl.ds(k * 256, 256)
        tmp_ref[rows, :] = gnode_ref[rows, :]
    pl.semaphore_wait(barrier, n - 1)

    def scatter(k):
        p = rank(k)
        return pltpu.make_async_remote_copy(
            src_ref=raw_ref.at[p], dst_ref=part_ref.at[k],
            send_sem=rs_send.at[k], recv_sem=rs_recv.at[k],
            device_id=device(p), device_id_type=MESH,
        )

    def spread(k):
        p = rank(k)
        return pltpu.make_async_remote_copy(
            src_ref=sum_ref, dst_ref=all_ref.at[me],
            send_sem=ag_send.at[k], recv_sem=ag_recv.at[k],
            device_id=device(p), device_id_type=MESH,
        )

    @pl.loop(1, n)
    def _(k):
        scatter(k).start()

    ids = neighbours()
    halos = []
    for d in range(6):
        halos.append(pltpu.make_async_remote_copy(
            src_ref=faces[d], dst_ref=lands[d],
            send_sem=halo_send.at[d], recv_sem=halo_recv.at[d],
            device_id=ids[d], device_id_type=MESH,
        ))
        halos[-1].start()

    @pl.loop(1, n)
    def _(k):
        scatter(k).wait_recv()

    def add(k, total):
        return total + part_ref[k].astype(F32)

    total = lax.fori_loop(1, n, add, raw_ref[me].astype(F32)).astype(BF16)
    sum_ref[...] = total
    all_ref[me] = total

    @pl.loop(1, n)
    def _(k):
        spread(k).start()

    for d in range(6):
        halos[d].wait_recv()
    tmp_ref[pl.ds(0, plane), :] += lands[0][...].astype(F32)
    tmp_ref[pl.ds(cells - plane, plane), :] += lands[1][...].astype(F32)
    low, high = lands[2][...].astype(F32), lands[3][...].astype(F32)
    for i in range(sx):
        tmp_ref[pl.ds(i * plane, sz), :] += low[i * sz:(i + 1) * sz]
        tmp_ref[pl.ds(i * plane + plane - sz, sz), :] += high[i * sz:(i + 1) * sz]
    tmp_ref[pl.ds(0, sx * sy, stride=sz), :] += lands[4][...].astype(F32)
    tmp_ref[pl.ds(sz - 1, sx * sy, stride=sz), :] += lands[5][...].astype(F32)
    for k in range(cells // 256):
        rows = pl.ds(k * 256, 256)
        gout_ref[rows, :] = tmp_ref[rows, :].astype(BF16)

    @pl.loop(1, n)
    def _(k):
        spread(k).wait_recv()

    full = all_ref[...].astype(F32).reshape(-1, h)
    squares = jnp.sum(jnp.sum(fold_rows(full * full), axis=0, keepdims=True), axis=1, keepdims=True)
    factor = 1.0 / jnp.maximum(1.0, jnp.sqrt(squares / (7 * h * h + 4 * h)))
    at = 0
    for ref in (w1e_ref, w2e_ref, w1n_ref, w2n_ref, bias_ref):
        rows = ref.shape[0]
        ref[...] = full[at:at + rows] * factor
        at += rows

    @pl.loop(1, n)
    def _(k):
        scatter(k).wait_send()
        spread(k).wait_send()

    for d in range(6):
        halos[d].wait_send()


def on_device(
    node_latent, edge_latent, senders, receivers,
    w1_edge, b1_edge, w2_edge, b2_edge, w1_node, b1_node, w2_node,
    cot_node, cot_edge,
):
    sx, sy, sz, lat = node_latent.shape
    cells = sx * sy * sz
    edges = edge_latent.shape[3]
    own = node_latent.reshape(cells, lat)
    vmem = pl.BlockSpec(memory_space=pltpu.VMEM)
    smem = pl.BlockSpec(memory_space=pltpu.SMEM)
    face_rows = [sy * sz, sy * sz, sx * sz, sx * sz, sx * sy, sx * sy]
    dims = (sx, sy, sz)
    faces = pl.pallas_call(
        functools.partial(halo_kernel, dims),
        out_shape=[jax.ShapeDtypeStruct((n, lat), BF16) for n in face_rows],
        in_specs=[vmem],
        out_specs=[vmem] * 6,
        scratch_shapes=[pltpu.VMEM((n, lat), BF16) for n in face_rows] * 2
        + [
            pltpu.VMEM((cells, lat), F32),
            pltpu.SemaphoreType.DMA((6,)),
            pltpu.SemaphoreType.DMA((6,)),
        ],
        compiler_params=pltpu.CompilerParams(collective_id=0, has_side_effects=True),
    )(own)
    r = receivers.reshape(edges)
    s = senders.reshape(edges)
    padded = ((r // (sy * sz) + 1) * (sy + 2) + r // sz % sy + 1) * (sz + 2) + r % sz + 1
    diff = s - padded
    step_x = (sy + 2) * (sz + 2)
    step_y = sz + 2
    direction = jnp.where(
        diff == step_x, 0,
        jnp.where(
            diff == -step_x, 1,
            jnp.where(
                diff == step_y, 2, jnp.where(diff == -step_y, 3, jnp.where(diff == 1, 4, 5))
            ),
        ),
    )
    stride = 1
    while stride < cells + WIDE:
        stride *= 2
    tiles = edges // TILE
    keys = (direction * stride + r).reshape(tiles, TILE)
    grouped = r.reshape(tiles, TILE)
    base = grouped[:, 0] // ROUND * ROUND
    counts = (grouped[:, -1] - base) // WIN + 1

    devices = 1
    for axis in AXES:
        devices *= lax.axis_size(axis)
    chunk = -(-(7 * lat + 4) // (16 * devices)) * 16
    outs = pl.pallas_call(
        functools.partial(layer_kernel, dims, stride),
        out_shape=[
            jax.ShapeDtypeStruct((cells, lat), F32),
            jax.ShapeDtypeStruct((edges, lat), BF16),
            jax.ShapeDtypeStruct((devices * chunk, lat), BF16),
        ] + [jax.ShapeDtypeStruct((n, lat), BF16) for n in face_rows],
        in_specs=[smem] * 2 + [vmem] * 18,
        out_specs=[vmem] * 9,
        scratch_shapes=[
            pltpu.VMEM((6, cells + WIDE, lat), BF16),
            pltpu.VMEM((cells, lat), F32),
            pltpu.VMEM((cells, lat), F32),
            pltpu.VMEM((cells, lat), F32),
            pltpu.VMEM((edges, lat), F32),
            pltpu.VMEM((cells + WIDE, lat), F32),
            pltpu.VMEM((cells + WIDE, lat), BF16),
            pltpu.VMEM((4, 8, lat), F32),
            pltpu.VMEM((lat, lat), F32),
            pltpu.VMEM((devices * chunk, lat), F32),
        ] + [pltpu.VMEM((cells + WIDE, lat), F32)] * 6,
        compiler_params=pltpu.CompilerParams(vmem_limit_bytes=60 * 1024 * 1024),
        cost_estimate=pl.CostEstimate(
            flops=40 * edges * lat * lat, bytes_accessed=6 * edges * lat, transcendentals=0
        ),
    )(
        base, counts,
        own, edge_latent.reshape(edges, lat), cot_edge.reshape(edges, lat),
        cot_node.reshape(cells, lat), keys,
        w1_edge, b1_edge.reshape(1, lat), w2_edge, b2_edge.reshape(1, lat),
        w1_node, b1_node.reshape(1, lat), w2_node,
        *faces,
    )
    gnode, gedge, raw = outs[:3]
    out = pl.pallas_call(
        functools.partial(reduce_kernel, dims),
        out_shape=[
            jax.ShapeDtypeStruct((cells, lat), BF16),
            jax.ShapeDtypeStruct((3 * lat, lat), F32),
            jax.ShapeDtypeStruct((lat, lat), F32),
            jax.ShapeDtypeStruct((2 * lat, lat), F32),
            jax.ShapeDtypeStruct((lat, lat), F32),
            jax.ShapeDtypeStruct((4, lat), F32),
        ],
        in_specs=[vmem] * 8,
        out_specs=[vmem] * 6,
        scratch_shapes=[
            pltpu.VMEM((devices, chunk, lat), BF16),
            pltpu.VMEM((chunk, lat), BF16),
            pltpu.VMEM((devices, chunk, lat), BF16),
            pltpu.VMEM((cells, lat), F32),
        ]
        + [pltpu.VMEM((n, lat), BF16) for n in face_rows]
        + [pltpu.SemaphoreType.DMA((devices,))] * 4
        + [pltpu.SemaphoreType.DMA((6,))] * 2,
        compiler_params=pltpu.CompilerParams(collective_id=1, has_side_effects=True),
    )(raw.reshape(devices, chunk, lat), gnode, *outs[3:])
    return (
        out[0].reshape(node_latent.shape),
        gedge.reshape(edge_latent.shape),
        *out[1:],
    )


def solution(mesh):
    cell = P("gx", "gy", "gz", None)
    edge = P("gx", "gy", "gz", None, None)
    return jax.shard_map(
        on_device,
        mesh=mesh,
        in_specs=(cell, edge, cell, cell, P(), P(), P(), P(), P(), P(), P(), cell, edge),
        out_specs=(cell, edge, P(), P(), P(), P(), P()),
        check_vma=False,
    )
```

```python
import functools

import jax
import jax.numpy as jnp
from jax import lax
from jax.experimental import pallas as pl
from jax.experimental.pallas import tpu as pltpu
from jax.sharding import PartitionSpec as P

F32 = jnp.float32
BF16 = jnp.bfloat16
TILE = 256
WIN = 80
WIDE = 128
ROUND = 16


def dot(left, right):
    return jnp.dot(left, right, preferred_element_type=F32)


def dot_t(left, right):
    return lax.dot_general(left, right, (((0,), (0,)), ((), ())), preferred_element_type=F32)


def dot_nt(left, right):
    return lax.dot_general(left, right, (((1,), (1,)), ((), ())), preferred_element_type=F32)


def sigma_of(values):
    return 0.5 + 0.5 * jnp.tanh(0.5 * values)


def fold_rows(values):
    return jnp.sum(values.reshape(-1, 8, values.shape[-1]), axis=0)


def layer_kernel(
    dims,
    stride,
    base_ref, count_ref,
    node_ref, edge_ref, cot_ref, cotn_ref, key_ref,
    w1e_ref, b1e_ref, w2e_ref, b2e_ref, w1n_ref, b1n_ref, w2n_ref,
    fxp_ref, fxm_ref, fyp_ref, fym_ref, fzp_ref, fzm_ref,
    gnode_ref, gedge_ref, rawb_ref,
    oxp_ref, oxm_ref, oyp_ref, oym_ref, ozp_ref, ozm_ref,
    tab_ref, s_ref, r_ref, tmp_ref, z_ref, agg_ref, dagg_ref, bias_ref, rawr_ref, raw_ref, *g_refs,
):
    sx, sy, sz = dims
    cells = sx * sy * sz
    plane = sy * sz
    lat = node_ref.shape[1]
    tiles = edge_ref.shape[0] // TILE
    h = lat
    slab = 256
    slabs = cells // slab

    w1s = w1e_ref[h:2 * h, :]
    w1r = w1e_ref[2 * h:, :]

    for k in range(slabs):
        rows = pl.ds(k * slab, slab)
        s_ref[rows, :] = dot(node_ref[rows, :], w1s)
        r_ref[rows, :] = dot(node_ref[rows, :], w1r) + b1e_ref[...]

    def publish(d):
        for k in range(slabs):
            rows = pl.ds(k * slab, slab)
            tab_ref[d, rows, :] = (tmp_ref[rows, :] + r_ref[rows, :]).astype(BF16)
        tab_ref[d, pl.ds(cells, WIDE), :] = jnp.zeros((WIDE, h), BF16)

    def shift_up(by):
        for k in range(slabs):
            n = min(slab, cells - by - k * slab)
            if n > 0:
                tmp_ref[pl.ds(k * slab, n), :] = s_ref[pl.ds(k * slab + by, n), :]

    def shift_down(by):
        for k in range(slabs):
            n = min(slab, cells - by - k * slab)
            if n > 0:
                tmp_ref[pl.ds(k * slab + by, n), :] = s_ref[pl.ds(k * slab, n), :]

    shift_up(plane)
    tmp_ref[pl.ds(cells - plane, plane), :] = dot(fxp_ref[...], w1s)
    publish(0)
    shift_down(plane)
    tmp_ref[pl.ds(0, plane), :] = dot(fxm_ref[...], w1s)
    publish(1)
    shift_up(sz)
    face = dot(fyp_ref[...], w1s)
    for i in range(sx):
        tmp_ref[pl.ds(i * plane + plane - sz, sz), :] = face[i * sz:(i + 1) * sz]
    publish(2)
    shift_down(sz)
    face = dot(fym_ref[...], w1s)
    for i in range(sx):
        tmp_ref[pl.ds(i * plane, sz), :] = face[i * sz:(i + 1) * sz]
    publish(3)
    shift_up(1)
    tmp_ref[pl.ds(sz - 1, sx * sy, stride=sz), :] = dot(fzp_ref[...], w1s)
    publish(4)
    shift_down(1)
    tmp_ref[pl.ds(0, sx * sy, stride=sz), :] = dot(fzm_ref[...], w1s)
    publish(5)

    for k in range(slabs):
        rows = pl.ds(k * slab, slab)
        agg_ref[rows, :] = jnp.zeros((slab, h), F32)
        for g_ref in g_refs:
            g_ref[rows, :] = jnp.zeros((slab, h), F32)
    agg_ref[pl.ds(cells, WIDE), :] = jnp.zeros((WIDE, h), F32)
    dagg_ref[pl.ds(cells, WIDE), :] = jnp.zeros((WIDE, h), BF16)
    for g_ref in g_refs:
        g_ref[pl.ds(cells, WIDE), :] = jnp.zeros((WIDE, h), F32)
    rawr_ref[...] = jnp.zeros_like(rawr_ref)
    bias_ref[...] = jnp.zeros_like(bias_ref)

    lane_chunks = (6 * WIN + 127) // 128

    def lane_values():
        out = []
        for q in range(lane_chunks):
            m = lax.broadcasted_iota(jnp.int32, (1, 128), 1) + 128 * q
            d = jnp.zeros((1, 128), jnp.int32)
            for k in range(1, 6):
                d = d + (m >= k * WIN).astype(jnp.int32)
            out.append(jnp.where(m < 6 * WIN, m + d * (stride - WIN), -(1 << 30)))
        return out

    def columns(row):
        parts = [
            jnp.broadcast_to(row[:, q * 128:(q + 1) * 128], (128, 128)).T
            for q in range(TILE // 128)
        ]
        return jnp.concatenate(parts, axis=0)

    def hot_cols(col, b):
        col = col - b
        pieces = [jnp.where(col == v, 1.0, 0.0).astype(BF16) for v in lane_values()]
        return jnp.concatenate(pieces, axis=1)

    def gather_table(col, b):
        pieces = [tab_ref[d, pl.ds(b, WIN), :] for d in range(6)]
        pad = lane_chunks * 128 - 6 * WIN
        if pad:
            pieces.append(jnp.zeros((pad, h), BF16))
        return dot(hot_cols(col, b), jnp.concatenate(pieces, axis=0))

    def hot_cell_rows(row, b, width):
        cell = (row & (stride - 1)) - b
        return jnp.where(
            lax.broadcasted_iota(jnp.int32, (width, TILE), 0) == cell, 1.0, 0.0
        ).astype(BF16)

    def hot_cell_cols(col, b, width):
        cell = (col & (stride - 1)) - b
        return jnp.where(
            lax.broadcasted_iota(jnp.int32, (TILE, width), 1) == cell, 1.0, 0.0
        ).astype(BF16)

    def hot_dir_rows(row, b):
        iota = lax.broadcasted_iota(jnp.int32, (WIN, TILE), 0)
        pieces = [
            jnp.where(iota == row - (b + d * stride), 1.0, 0.0).astype(BF16) for d in range(6)
        ]
        return jnp.concatenate(pieces, axis=0)

    w1a = w1e_ref[:h, :]

    def forward_tile(t, slow):
        rows = pl.ds(pl.multiple_of(t * TILE, TILE), TILE)
        b = pl.multiple_of(base_ref[t], ROUND)
        row = key_ref[pl.ds(t, 1), :]
        col = columns(row)
        e = edge_ref[rows, :]
        z = dot(e, w1a) + gather_table(col, b)
        z_ref[rows, :] = z
        if slow:
            @pl.loop(1, count_ref[t])
            def _(w):
                z_ref[rows, :] += gather_table(col, pl.multiple_of(b + w * WIN, ROUND))
            z = z_ref[rows, :]
        u = (z * sigma_of(z)).astype(BF16)
        fresh = (e.astype(F32) + dot(u, w2e_ref[...]) + b2e_ref[...]).astype(BF16)

        def scatter(at):
            agg_ref[pl.ds(at, WIN), :] += dot(hot_cell_rows(row, at, WIN), fresh)

        scatter(b)
        if slow:
            @pl.loop(1, count_ref[t])
            def _(w):
                scatter(pl.multiple_of(b + w * WIN, ROUND))

    def backward_tile(t, slow):
        rows = pl.ds(pl.multiple_of(t * TILE, TILE), TILE)
        b = pl.multiple_of(base_ref[t], ROUND)
        row = key_ref[pl.ds(t, 1), :]
        col = columns(row)

        def gather(at):
            hot = hot_cell_cols(col, at, WIDE)
            if slow:
                keep = lax.broadcasted_iota(jnp.int32, (1, WIDE), 1) < WIN
                hot = jnp.where(keep, hot.astype(F32), 0.0).astype(BF16)
            return dot(hot, dagg_ref[pl.ds(at, WIDE), :])

        back = gather(b)
        if slow:
            def more(w, back):
                return back + gather(pl.multiple_of(b + w * WIN, ROUND))
            back = lax.fori_loop(1, count_ref[t], more, back)
        e = edge_ref[rows, :]
        d = (cot_ref[rows, :].astype(F32) + back).astype(BF16)
        z = z_ref[rows, :]
        s = sigma_of(z)
        u = z * s
        slope = s * (1.0 + z * (1.0 - s))
        dz = dot_nt(d, w2e_ref[...]) * slope
        dzb = dz.astype(BF16)
        gedge_ref[rows, :] = (d.astype(F32) + dot_nt(dzb, w1a)).astype(BF16)

        def scatter(at):
            out = dot(hot_dir_rows(row, at), dzb)
            for k, g_ref in enumerate(g_refs):
                g_ref[pl.ds(at, WIN), :] += out[k * WIN:(k + 1) * WIN]

        scatter(b)
        if slow:
            @pl.loop(1, count_ref[t])
            def _(w):
                scatter(pl.multiple_of(b + w * WIN, ROUND))
        raw_ref[0:h, :] += dot_t(e, dzb)
        raw_ref[3 * h:4 * h, :] += dot_t(u.astype(BF16), d)
        bias_ref[0] += fold_rows(dzb.astype(F32))
        bias_ref[1] += fold_rows(d.astype(F32))

    raw_ref[...] = jnp.zeros_like(raw_ref)
    most = lax.fori_loop(0, tiles, lambda t, m: jnp.maximum(m, count_ref[t]), 1)

    @pl.when(most == 1)
    def _():
        @pl.loop(0, tiles, unroll=2)
        def _(t):
            forward_tile(t, False)

    @pl.when(most > 1)
    def _():
        @pl.loop(0, tiles)
        def _(t):
            forward_tile(t, True)

    at = 4 * h

    @pl.loop(0, slabs)
    def _(k):
        rows = pl.ds(pl.multiple_of(k * slab, slab), slab)
        own = node_ref[rows, :]
        agg = agg_ref[rows, :].astype(BF16)
        cot = cotn_ref[rows, :]
        z = dot(own, w1n_ref[:h, :]) + dot(agg, w1n_ref[h:, :]) + b1n_ref[...]
        s = sigma_of(z)
        u = (z * s).astype(BF16)
        dz = (dot_nt(cot, w2n_ref[...]) * (s * (1.0 + z * (1.0 - s)))).astype(BF16)
        gnode_ref[rows, :] = cot.astype(F32) + dot_nt(dz, w1n_ref[:h, :])
        dagg_ref[rows, :] = dot_nt(dz, w1n_ref[h:, :]).astype(BF16)
        raw_ref[at:at + h, :] += dot_t(own, dz)
        raw_ref[at + h:at + 2 * h, :] += dot_t(agg, dz)
        raw_ref[at + 2 * h:at + 3 * h, :] += dot_t(u, cot)
        bias_ref[2] += fold_rows(dz.astype(F32))
        bias_ref[3] += fold_rows(cot.astype(F32))

    @pl.when(most == 1)
    def _():
        @pl.loop(0, tiles, unroll=2)
        def _(t):
            backward_tile(t, False)

    @pl.when(most > 1)
    def _():
        @pl.loop(0, tiles)
        def _(t):
            backward_tile(t, True)

    g0, g1, g2, g3, g4, g5 = g_refs
    for k in range(slabs):
        rows = pl.ds(k * slab, slab)
        total = g0[rows, :] + g1[rows, :] + g2[rows, :] + g3[rows, :] + g4[rows, :] + g5[rows, :]
        total = total.astype(BF16)
        gnode_ref[rows, :] += dot_nt(total, w1r)
        rawr_ref[...] += dot_t(node_ref[rows, :], total)
    raw_ref[2 * h:3 * h, :] = rawr_ref[...]

    acc = jnp.zeros((h, h), F32)

    def out_face(values, own_ref, out_ref):
        values = values.astype(BF16)
        out_ref[...] = dot_nt(values, w1s).astype(BF16)
        return dot_t(own_ref[...], values)

    acc += out_face(g0[pl.ds(cells - plane, plane), :], fxp_ref, oxp_ref)
    acc += out_face(g1[pl.ds(0, plane), :], fxm_ref, oxm_ref)
    pieces = [g2[pl.ds(i * plane + plane - sz, sz), :] for i in range(sx)]
    acc += out_face(jnp.concatenate(pieces, axis=0), fyp_ref, oyp_ref)
    pieces = [g3[pl.ds(i * plane, sz), :] for i in range(sx)]
    acc += out_face(jnp.concatenate(pieces, axis=0), fym_ref, oym_ref)
    acc += out_face(g4[pl.ds(sz - 1, sx * sy, stride=sz), :], fzp_ref, ozp_ref)
    acc += out_face(g5[pl.ds(0, sx * sy, stride=sz), :], fzm_ref, ozm_ref)
    for i in range(sx):
        g2[pl.ds(i * plane + plane - sz, sz), :] = jnp.zeros((sz, h), F32)
        g3[pl.ds(i * plane, sz), :] = jnp.zeros((sz, h), F32)
    g4[pl.ds(sz - 1, sx * sy, stride=sz), :] = jnp.zeros((sx * sy, h), F32)
    g5[pl.ds(0, sx * sy, stride=sz), :] = jnp.zeros((sx * sy, h), F32)

    tmp_ref[...] = jnp.zeros_like(tmp_ref)
    for g_ref, by in ((g0, plane), (g2, sz), (g4, 1)):
        for k in range(slabs):
            n = min(slab, cells - by - k * slab)
            if n > 0:
                tmp_ref[pl.ds(k * slab + by, n), :] += g_ref[pl.ds(k * slab, n), :]
    for g_ref, by in ((g1, plane), (g3, sz), (g5, 1)):
        for k in range(slabs):
            n = min(slab, cells - by - k * slab)
            if n > 0:
                tmp_ref[pl.ds(k * slab, n), :] += g_ref[pl.ds(k * slab + by, n), :]
    rawr_ref[...] = acc
    for k in range(slabs):
        rows = pl.ds(k * slab, slab)
        total = tmp_ref[rows, :].astype(BF16)
        gnode_ref[rows, :] += dot_nt(total, w1s)
        rawr_ref[...] += dot_t(node_ref[rows, :], total)
    raw_ref[h:2 * h, :] = rawr_ref[...]
    for k in range(4):
        raw_ref[7 * h + k:7 * h + k + 1, :] = jnp.sum(bias_ref[k], axis=0, keepdims=True)
    rawb_ref[...] = raw_ref[...].astype(BF16)


MESH = pl.DeviceIdType.MESH
AXES = ("gx", "gy", "gz")


def neighbours():
    here = [lax.axis_index(a) for a in AXES]
    out = []
    for k, a in enumerate(AXES):
        count = lax.axis_size(a)
        for step in (1, count - 1):
            at = list(here)
            at[k] = lax.rem(here[k] + step, count)
            out.append(tuple(at))
    return out


def halo_kernel(dims, node_ref, *refs):
    outs, sends, lands, tmp_ref, send_sem, recv_sem = (
        refs[:6], refs[6:12], refs[12:18], refs[18], refs[19], refs[20]
    )
    sx, sy, sz = dims
    plane = sy * sz
    cells = sx * plane
    ids = neighbours()
    barrier = pltpu.get_barrier_semaphore()
    for who in ids:
        pl.semaphore_signal(barrier, inc=1, device_id=who, device_id_type=MESH)
    for k in range(cells // 256):
        rows = pl.ds(k * 256, 256)
        tmp_ref[rows, :] = node_ref[rows, :].astype(F32)
    sends[4][...] = tmp_ref[pl.ds(sz - 1, sx * sy, stride=sz), :].astype(BF16)
    sends[5][...] = tmp_ref[pl.ds(0, sx * sy, stride=sz), :].astype(BF16)
    sends[0][...] = node_ref[pl.ds(cells - plane, plane), :]
    sends[1][...] = node_ref[pl.ds(0, plane), :]
    sends[2][...] = jnp.concatenate(
        [tmp_ref[pl.ds(i * plane + plane - sz, sz), :] for i in range(sx)], axis=0
    ).astype(BF16)
    sends[3][...] = jnp.concatenate(
        [tmp_ref[pl.ds(i * plane, sz), :] for i in range(sx)], axis=0
    ).astype(BF16)
    pl.semaphore_wait(barrier, 6)
    copies = []
    for d in (4, 5, 0, 1, 2, 3):
        copy = pltpu.make_async_remote_copy(
            src_ref=sends[d], dst_ref=lands[d ^ 1],
            send_sem=send_sem.at[d], recv_sem=recv_sem.at[d ^ 1],
            device_id=ids[d], device_id_type=MESH,
        )
        copy.start()
        copies.append((d, copy))
    for d, copy in copies:
        copy.wait_send()
    for d, copy in copies:
        copy.wait_recv()
        outs[d ^ 1][...] = lands[d ^ 1][...]


def reduce_kernel(dims, raw_ref, gnode_ref, *refs):
    faces = refs[:6]
    gout_ref, allout_ref = refs[6:8]
    part_ref, sum_ref, all_ref, tmp_ref = refs[8:12]
    lands = refs[12:18]
    rs_send, rs_recv, ag_send, ag_recv, halo_send, halo_recv = refs[18:24]
    sx, sy, sz = dims
    plane = sy * sz
    cells = sx * plane
    h = gnode_ref.shape[1]
    nx, ny, nz = [lax.axis_size(a) for a in AXES]
    n = nx * ny * nz
    ix, iy, iz = [lax.axis_index(a) for a in AXES]
    me = (ix * ny + iy) * nz + iz

    def rank(k):
        return lax.rem(me + k, n)

    def device(p):
        return (p // (ny * nz), p // nz % ny, p % nz)

    barrier = pltpu.get_barrier_semaphore()

    @pl.loop(1, n)
    def _(k):
        pl.semaphore_signal(barrier, inc=1, device_id=device(rank(k)), device_id_type=MESH)

    for k in range(cells // 256):
        rows = pl.ds(k * 256, 256)
        tmp_ref[rows, :] = gnode_ref[rows, :]
    pl.semaphore_wait(barrier, n - 1)

    def scatter(k):
        p = rank(k)
        return pltpu.make_async_remote_copy(
            src_ref=raw_ref.at[p], dst_ref=part_ref.at[k],
            send_sem=rs_send.at[k], recv_sem=rs_recv.at[k],
            device_id=device(p), device_id_type=MESH,
        )

    def spread(k):
        p = rank(k)
        return pltpu.make_async_remote_copy(
            src_ref=sum_ref, dst_ref=all_ref.at[me],
            send_sem=ag_send.at[k], recv_sem=ag_recv.at[k],
            device_id=device(p), device_id_type=MESH,
        )

    @pl.loop(1, n)
    def _(k):
        scatter(k).start()

    ids = neighbours()
    halos = []
    for d in range(6):
        halos.append(pltpu.make_async_remote_copy(
            src_ref=faces[d], dst_ref=lands[d],
            send_sem=halo_send.at[d], recv_sem=halo_recv.at[d],
            device_id=ids[d], device_id_type=MESH,
        ))
        halos[-1].start()

    @pl.loop(1, n)
    def _(k):
        scatter(k).wait_recv()

    def add(k, total):
        return total + part_ref[k].astype(F32)

    total = lax.fori_loop(1, n, add, raw_ref[me].astype(F32)).astype(BF16)
    sum_ref[...] = total
    all_ref[me] = total

    @pl.loop(1, n)
    def _(k):
        spread(k).start()

    for d in range(6):
        halos[d].wait_recv()
    tmp_ref[pl.ds(0, plane), :] += lands[0][...].astype(F32)
    tmp_ref[pl.ds(cells - plane, plane), :] += lands[1][...].astype(F32)
    low, high = lands[2][...].astype(F32), lands[3][...].astype(F32)
    for i in range(sx):
        tmp_ref[pl.ds(i * plane, sz), :] += low[i * sz:(i + 1) * sz]
        tmp_ref[pl.ds(i * plane + plane - sz, sz), :] += high[i * sz:(i + 1) * sz]
    tmp_ref[pl.ds(0, sx * sy, stride=sz), :] += lands[4][...].astype(F32)
    tmp_ref[pl.ds(sz - 1, sx * sy, stride=sz), :] += lands[5][...].astype(F32)
    for k in range(cells // 256):
        rows = pl.ds(k * 256, 256)
        gout_ref[rows, :] = tmp_ref[rows, :].astype(BF16)

    @pl.loop(1, n)
    def _(k):
        spread(k).wait_recv()

    allout_ref[...] = all_ref[...]

    @pl.loop(1, n)
    def _(k):
        scatter(k).wait_send()
        spread(k).wait_send()

    for d in range(6):
        halos[d].wait_send()


def finish_kernel(all_ref, gin_ref, gout_ref, w1e_ref, w2e_ref, w1n_ref, w2n_ref, bias_ref):
    h = gin_ref.shape[1]
    gout_ref[...] = gin_ref[...]
    full = all_ref[...].astype(F32).reshape(-1, h)
    squares = jnp.sum(jnp.sum(fold_rows(full * full), axis=0, keepdims=True), axis=1, keepdims=True)
    factor = 1.0 / jnp.maximum(1.0, jnp.sqrt(squares / (7 * h * h + 4 * h)))
    at = 0
    for ref in (w1e_ref, w2e_ref, w1n_ref, w2n_ref, bias_ref):
        rows = ref.shape[0]
        ref[...] = full[at:at + rows] * factor
        at += rows


def on_device(
    node_latent, edge_latent, senders, receivers,
    w1_edge, b1_edge, w2_edge, b2_edge, w1_node, b1_node, w2_node,
    cot_node, cot_edge,
):
    sx, sy, sz, lat = node_latent.shape
    cells = sx * sy * sz
    edges = edge_latent.shape[3]
    own = node_latent.reshape(cells, lat)
    vmem = pl.BlockSpec(memory_space=pltpu.VMEM)
    smem = pl.BlockSpec(memory_space=pltpu.SMEM)
    face_rows = [sy * sz, sy * sz, sx * sz, sx * sz, sx * sy, sx * sy]
    dims = (sx, sy, sz)
    faces = pl.pallas_call(
        functools.partial(halo_kernel, dims),
        out_shape=[jax.ShapeDtypeStruct((n, lat), BF16) for n in face_rows],
        in_specs=[vmem],
        out_specs=[vmem] * 6,
        scratch_shapes=[pltpu.VMEM((n, lat), BF16) for n in face_rows] * 2
        + [
            pltpu.VMEM((cells, lat), F32),
            pltpu.SemaphoreType.DMA((6,)),
            pltpu.SemaphoreType.DMA((6,)),
        ],
        compiler_params=pltpu.CompilerParams(collective_id=0, has_side_effects=True),
    )(own)
    r = receivers.reshape(edges)
    s = senders.reshape(edges)
    padded = ((r // (sy * sz) + 1) * (sy + 2) + r // sz % sy + 1) * (sz + 2) + r % sz + 1
    diff = s - padded
    step_x = (sy + 2) * (sz + 2)
    step_y = sz + 2
    direction = jnp.where(
        diff == step_x, 0,
        jnp.where(
            diff == -step_x, 1,
            jnp.where(
                diff == step_y, 2, jnp.where(diff == -step_y, 3, jnp.where(diff == 1, 4, 5))
            ),
        ),
    )
    stride = 1
    while stride < cells + WIDE:
        stride *= 2
    tiles = edges // TILE
    keys = (direction * stride + r).reshape(tiles, TILE)
    grouped = r.reshape(tiles, TILE)
    base = grouped[:, 0] // ROUND * ROUND
    counts = (grouped[:, -1] - base) // WIN + 1

    devices = 1
    for axis in AXES:
        devices *= lax.axis_size(axis)
    chunk = -(-(7 * lat + 4) // (16 * devices)) * 16
    outs = pl.pallas_call(
        functools.partial(layer_kernel, dims, stride),
        out_shape=[
            jax.ShapeDtypeStruct((cells, lat), F32),
            jax.ShapeDtypeStruct((edges, lat), BF16),
            jax.ShapeDtypeStruct((devices * chunk, lat), BF16),
        ] + [jax.ShapeDtypeStruct((n, lat), BF16) for n in face_rows],
        in_specs=[smem] * 2 + [vmem] * 18,
        out_specs=[vmem] * 9,
        scratch_shapes=[
            pltpu.VMEM((6, cells + WIDE, lat), BF16),
            pltpu.VMEM((cells, lat), F32),
            pltpu.VMEM((cells, lat), F32),
            pltpu.VMEM((cells, lat), F32),
            pltpu.VMEM((edges, lat), F32),
            pltpu.VMEM((cells + WIDE, lat), F32),
            pltpu.VMEM((cells + WIDE, lat), BF16),
            pltpu.VMEM((4, 8, lat), F32),
            pltpu.VMEM((lat, lat), F32),
            pltpu.VMEM((devices * chunk, lat), F32),
        ] + [pltpu.VMEM((cells + WIDE, lat), F32)] * 6,
        compiler_params=pltpu.CompilerParams(vmem_limit_bytes=60 * 1024 * 1024),
        cost_estimate=pl.CostEstimate(
            flops=40 * edges * lat * lat, bytes_accessed=6 * edges * lat, transcendentals=0
        ),
    )(
        base, counts,
        own, edge_latent.reshape(edges, lat), cot_edge.reshape(edges, lat),
        cot_node.reshape(cells, lat), keys,
        w1_edge, b1_edge.reshape(1, lat), w2_edge, b2_edge.reshape(1, lat),
        w1_node, b1_node.reshape(1, lat), w2_node,
        *faces,
    )
    gnode, gedge, raw = outs[:3]
    gsum, full = pl.pallas_call(
        functools.partial(reduce_kernel, dims),
        out_shape=[
            jax.ShapeDtypeStruct((cells, lat), BF16),
            jax.ShapeDtypeStruct((devices, chunk, lat), BF16),
        ],
        in_specs=[vmem] * 8,
        out_specs=[vmem] * 2,
        scratch_shapes=[
            pltpu.VMEM((devices, chunk, lat), BF16),
            pltpu.VMEM((chunk, lat), BF16),
            pltpu.VMEM((devices, chunk, lat), BF16),
            pltpu.VMEM((cells, lat), F32),
        ]
        + [pltpu.VMEM((n, lat), BF16) for n in face_rows]
        + [pltpu.SemaphoreType.DMA((devices,))] * 4
        + [pltpu.SemaphoreType.DMA((6,))] * 2,
        compiler_params=pltpu.CompilerParams(collective_id=1, has_side_effects=True),
    )(raw.reshape(devices, chunk, lat), gnode, *outs[3:])
    out = pl.pallas_call(
        finish_kernel,
        out_shape=[
            jax.ShapeDtypeStruct((cells, lat), BF16),
            jax.ShapeDtypeStruct((3 * lat, lat), F32),
            jax.ShapeDtypeStruct((lat, lat), F32),
            jax.ShapeDtypeStruct((2 * lat, lat), F32),
            jax.ShapeDtypeStruct((lat, lat), F32),
            jax.ShapeDtypeStruct((4, lat), F32),
        ],
        in_specs=[vmem] * 2,
        out_specs=[vmem] * 6,
    )(full, gsum)
    return (
        out[0].reshape(node_latent.shape),
        gedge.reshape(edge_latent.shape),
        *out[1:],
    )


def solution(mesh):
    cell = P("gx", "gy", "gz", None)
    edge = P("gx", "gy", "gz", None, None)
    return jax.shard_map(
        on_device,
        mesh=mesh,
        in_specs=(cell, edge, cell, cell, P(), P(), P(), P(), P(), P(), P(), cell, edge),
        out_specs=(cell, edge, P(), P(), P(), P(), P()),
        check_vma=False,
    )
```

```python
import functools

import jax
import jax.numpy as jnp
from jax import lax
from jax.experimental import pallas as pl
from jax.experimental.pallas import tpu as pltpu
from jax.sharding import PartitionSpec as P

F32 = jnp.float32
BF16 = jnp.bfloat16
TILE = 256
WIN = 80
WIDE = 128
ROUND = 16


def dot(left, right):
    return jnp.dot(left, right, preferred_element_type=F32)


def dot_t(left, right):
    return lax.dot_general(left, right, (((0,), (0,)), ((), ())), preferred_element_type=F32)


def dot_nt(left, right):
    return lax.dot_general(left, right, (((1,), (1,)), ((), ())), preferred_element_type=F32)


def sigma_of(values):
    return 0.5 + 0.5 * jnp.tanh(0.5 * values)


def fold_rows(values):
    return jnp.sum(values.reshape(-1, 8, values.shape[-1]), axis=0)


def layer_kernel(
    dims,
    stride,
    base_ref, count_ref,
    node_ref, edge_ref, cot_ref, cotn_ref, key_ref,
    w1e_ref, b1e_ref, w2e_ref, b2e_ref, w1n_ref, b1n_ref, w2n_ref,
    fxp_ref, fxm_ref, fyp_ref, fym_ref, fzp_ref, fzm_ref,
    gnode_ref, gedge_ref, rawb_ref,
    oxp_ref, oxm_ref, oyp_ref, oym_ref, ozp_ref, ozm_ref,
    tab_ref, s_ref, r_ref, tmp_ref, z_ref, agg_ref, dagg_ref, bias_ref, rawr_ref, raw_ref, *g_refs,
):
    sx, sy, sz = dims
    cells = sx * sy * sz
    plane = sy * sz
    lat = node_ref.shape[1]
    tiles = edge_ref.shape[0] // TILE
    h = lat
    slab = 256
    slabs = cells // slab

    w1s = w1e_ref[h:2 * h, :]
    w1r = w1e_ref[2 * h:, :]

    for k in range(slabs):
        rows = pl.ds(k * slab, slab)
        s_ref[rows, :] = dot(node_ref[rows, :], w1s)
        r_ref[rows, :] = dot(node_ref[rows, :], w1r) + b1e_ref[...]

    def publish(d):
        for k in range(slabs):
            rows = pl.ds(k * slab, slab)
            tab_ref[d, rows, :] = (tmp_ref[rows, :] + r_ref[rows, :]).astype(BF16)
        tab_ref[d, pl.ds(cells, WIDE), :] = jnp.zeros((WIDE, h), BF16)

    def shift_up(by):
        for k in range(slabs):
            n = min(slab, cells - by - k * slab)
            if n > 0:
                tmp_ref[pl.ds(k * slab, n), :] = s_ref[pl.ds(k * slab + by, n), :]

    def shift_down(by):
        for k in range(slabs):
            n = min(slab, cells - by - k * slab)
            if n > 0:
                tmp_ref[pl.ds(k * slab + by, n), :] = s_ref[pl.ds(k * slab, n), :]

    shift_up(plane)
    tmp_ref[pl.ds(cells - plane, plane), :] = dot(fxp_ref[...], w1s)
    publish(0)
    shift_down(plane)
    tmp_ref[pl.ds(0, plane), :] = dot(fxm_ref[...], w1s)
    publish(1)
    shift_up(sz)
    face = dot(fyp_ref[...], w1s)
    for i in range(sx):
        tmp_ref[pl.ds(i * plane + plane - sz, sz), :] = face[i * sz:(i + 1) * sz]
    publish(2)
    shift_down(sz)
    face = dot(fym_ref[...], w1s)
    for i in range(sx):
        tmp_ref[pl.ds(i * plane, sz), :] = face[i * sz:(i + 1) * sz]
    publish(3)
    shift_up(1)
    tmp_ref[pl.ds(sz - 1, sx * sy, stride=sz), :] = dot(fzp_ref[...], w1s)
    publish(4)
    shift_down(1)
    tmp_ref[pl.ds(0, sx * sy, stride=sz), :] = dot(fzm_ref[...], w1s)
    publish(5)

    for k in range(slabs):
        rows = pl.ds(k * slab, slab)
        agg_ref[rows, :] = jnp.zeros((slab, h), F32)
        for g_ref in g_refs:
            g_ref[rows, :] = jnp.zeros((slab, h), F32)
    agg_ref[pl.ds(cells, WIDE), :] = jnp.zeros((WIDE, h), F32)
    dagg_ref[pl.ds(cells, WIDE), :] = jnp.zeros((WIDE, h), BF16)
    for g_ref in g_refs:
        g_ref[pl.ds(cells, WIDE), :] = jnp.zeros((WIDE, h), F32)
    rawr_ref[...] = jnp.zeros_like(rawr_ref)
    bias_ref[...] = jnp.zeros_like(bias_ref)

    lane_chunks = (6 * WIN + 127) // 128

    def lane_values():
        out = []
        for q in range(lane_chunks):
            m = lax.broadcasted_iota(jnp.int32, (1, 128), 1) + 128 * q
            d = jnp.zeros((1, 128), jnp.int32)
            for k in range(1, 6):
                d = d + (m >= k * WIN).astype(jnp.int32)
            out.append(jnp.where(m < 6 * WIN, m + d * (stride - WIN), -(1 << 30)))
        return out

    def columns(row):
        parts = [
            jnp.broadcast_to(row[:, q * 128:(q + 1) * 128], (128, 128)).T
            for q in range(TILE // 128)
        ]
        return jnp.concatenate(parts, axis=0)

    def hot_cols(col, b):
        col = col - b
        pieces = [jnp.where(col == v, 1.0, 0.0).astype(BF16) for v in lane_values()]
        return jnp.concatenate(pieces, axis=1)

    def gather_table(col, b):
        pieces = [tab_ref[d, pl.ds(b, WIN), :] for d in range(6)]
        pad = lane_chunks * 128 - 6 * WIN
        if pad:
            pieces.append(jnp.zeros((pad, h), BF16))
        return dot(hot_cols(col, b), jnp.concatenate(pieces, axis=0))

    def hot_cell_rows(row, b, width):
        cell = (row & (stride - 1)) - b
        return jnp.where(
            lax.broadcasted_iota(jnp.int32, (width, TILE), 0) == cell, 1.0, 0.0
        ).astype(BF16)

    def hot_cell_cols(col, b, width):
        cell = (col & (stride - 1)) - b
        return jnp.where(
            lax.broadcasted_iota(jnp.int32, (TILE, width), 1) == cell, 1.0, 0.0
        ).astype(BF16)

    def hot_dir_rows(row, b):
        iota = lax.broadcasted_iota(jnp.int32, (WIN, TILE), 0)
        pieces = [
            jnp.where(iota == row - (b + d * stride), 1.0, 0.0).astype(BF16) for d in range(6)
        ]
        return jnp.concatenate(pieces, axis=0)

    w1a = w1e_ref[:h, :]

    def forward_tile(t, slow):
        rows = pl.ds(pl.multiple_of(t * TILE, TILE), TILE)
        b = pl.multiple_of(base_ref[t], ROUND)
        row = key_ref[pl.ds(t, 1), :]
        col = columns(row)
        e = edge_ref[rows, :]
        z = dot(e, w1a) + gather_table(col, b)
        z_ref[rows, :] = z
        if slow:
            @pl.loop(1, count_ref[t])
            def _(w):
                z_ref[rows, :] += gather_table(col, pl.multiple_of(b + w * WIN, ROUND))
            z = z_ref[rows, :]
        u = (z * sigma_of(z)).astype(BF16)
        fresh = (e.astype(F32) + dot(u, w2e_ref[...]) + b2e_ref[...]).astype(BF16)

        def scatter(at):
            agg_ref[pl.ds(at, WIN), :] += dot(hot_cell_rows(row, at, WIN), fresh)

        scatter(b)
        if slow:
            @pl.loop(1, count_ref[t])
            def _(w):
                scatter(pl.multiple_of(b + w * WIN, ROUND))

    def backward_tile(t, slow):
        rows = pl.ds(pl.multiple_of(t * TILE, TILE), TILE)
        b = pl.multiple_of(base_ref[t], ROUND)
        row = key_ref[pl.ds(t, 1), :]
        col = columns(row)

        def gather(at):
            hot = hot_cell_cols(col, at, WIDE)
            if slow:
                keep = lax.broadcasted_iota(jnp.int32, (1, WIDE), 1) < WIN
                hot = jnp.where(keep, hot.astype(F32), 0.0).astype(BF16)
            return dot(hot, dagg_ref[pl.ds(at, WIDE), :])

        back = gather(b)
        if slow:
            def more(w, back):
                return back + gather(pl.multiple_of(b + w * WIN, ROUND))
            back = lax.fori_loop(1, count_ref[t], more, back)
        e = edge_ref[rows, :]
        d = (cot_ref[rows, :].astype(F32) + back).astype(BF16)
        z = z_ref[rows, :]
        s = sigma_of(z)
        u = z * s
        slope = s * (1.0 + z * (1.0 - s))
        dz = dot_nt(d, w2e_ref[...]) * slope
        dzb = dz.astype(BF16)
        gedge_ref[rows, :] = (d.astype(F32) + dot_nt(dzb, w1a)).astype(BF16)

        def scatter(at):
            out = dot(hot_dir_rows(row, at), dzb)
            for k, g_ref in enumerate(g_refs):
                g_ref[pl.ds(at, WIN), :] += out[k * WIN:(k + 1) * WIN]

        scatter(b)
        if slow:
            @pl.loop(1, count_ref[t])
            def _(w):
                scatter(pl.multiple_of(b + w * WIN, ROUND))
        raw_ref[0:h, :] += dot_t(e, dzb)
        raw_ref[3 * h:4 * h, :] += dot_t(u.astype(BF16), d)
        bias_ref[0] += fold_rows(dzb.astype(F32))
        bias_ref[1] += fold_rows(d.astype(F32))

    raw_ref[...] = jnp.zeros_like(raw_ref)
    most = lax.fori_loop(0, tiles, lambda t, m: jnp.maximum(m, count_ref[t]), 1)

    @pl.when(most == 1)
    def _():
        @pl.loop(0, tiles, unroll=4)
        def _(t):
            forward_tile(t, False)

    @pl.when(most > 1)
    def _():
        @pl.loop(0, tiles)
        def _(t):
            forward_tile(t, True)

    at = 4 * h

    @pl.loop(0, slabs)
    def _(k):
        rows = pl.ds(pl.multiple_of(k * slab, slab), slab)
        own = node_ref[rows, :]
        agg = agg_ref[rows, :].astype(BF16)
        cot = cotn_ref[rows, :]
        z = dot(own, w1n_ref[:h, :]) + dot(agg, w1n_ref[h:, :]) + b1n_ref[...]
        s = sigma_of(z)
        u = (z * s).astype(BF16)
        dz = (dot_nt(cot, w2n_ref[...]) * (s * (1.0 + z * (1.0 - s)))).astype(BF16)
        gnode_ref[rows, :] = cot.astype(F32) + dot_nt(dz, w1n_ref[:h, :])
        dagg_ref[rows, :] = dot_nt(dz, w1n_ref[h:, :]).astype(BF16)
        raw_ref[at:at + h, :] += dot_t(own, dz)
        raw_ref[at + h:at + 2 * h, :] += dot_t(agg, dz)
        raw_ref[at + 2 * h:at + 3 * h, :] += dot_t(u, cot)
        bias_ref[2] += fold_rows(dz.astype(F32))
        bias_ref[3] += fold_rows(cot.astype(F32))

    @pl.when(most == 1)
    def _():
        @pl.loop(0, tiles, unroll=4)
        def _(t):
            backward_tile(t, False)

    @pl.when(most > 1)
    def _():
        @pl.loop(0, tiles)
        def _(t):
            backward_tile(t, True)

    g0, g1, g2, g3, g4, g5 = g_refs
    for k in range(slabs):
        rows = pl.ds(k * slab, slab)
        total = g0[rows, :] + g1[rows, :] + g2[rows, :] + g3[rows, :] + g4[rows, :] + g5[rows, :]
        total = total.astype(BF16)
        gnode_ref[rows, :] += dot_nt(total, w1r)
        rawr_ref[...] += dot_t(node_ref[rows, :], total)
    raw_ref[2 * h:3 * h, :] = rawr_ref[...]

    acc = jnp.zeros((h, h), F32)

    def out_face(values, own_ref, out_ref):
        values = values.astype(BF16)
        out_ref[...] = dot_nt(values, w1s).astype(BF16)
        return dot_t(own_ref[...], values)

    acc += out_face(g0[pl.ds(cells - plane, plane), :], fxp_ref, oxp_ref)
    acc += out_face(g1[pl.ds(0, plane), :], fxm_ref, oxm_ref)
    pieces = [g2[pl.ds(i * plane + plane - sz, sz), :] for i in range(sx)]
    acc += out_face(jnp.concatenate(pieces, axis=0), fyp_ref, oyp_ref)
    pieces = [g3[pl.ds(i * plane, sz), :] for i in range(sx)]
    acc += out_face(jnp.concatenate(pieces, axis=0), fym_ref, oym_ref)
    acc += out_face(g4[pl.ds(sz - 1, sx * sy, stride=sz), :], fzp_ref, ozp_ref)
    acc += out_face(g5[pl.ds(0, sx * sy, stride=sz), :], fzm_ref, ozm_ref)
    for i in range(sx):
        g2[pl.ds(i * plane + plane - sz, sz), :] = jnp.zeros((sz, h), F32)
        g3[pl.ds(i * plane, sz), :] = jnp.zeros((sz, h), F32)
    g4[pl.ds(sz - 1, sx * sy, stride=sz), :] = jnp.zeros((sx * sy, h), F32)
    g5[pl.ds(0, sx * sy, stride=sz), :] = jnp.zeros((sx * sy, h), F32)

    tmp_ref[...] = jnp.zeros_like(tmp_ref)
    for g_ref, by in ((g0, plane), (g2, sz), (g4, 1)):
        for k in range(slabs):
            n = min(slab, cells - by - k * slab)
            if n > 0:
                tmp_ref[pl.ds(k * slab + by, n), :] += g_ref[pl.ds(k * slab, n), :]
    for g_ref, by in ((g1, plane), (g3, sz), (g5, 1)):
        for k in range(slabs):
            n = min(slab, cells - by - k * slab)
            if n > 0:
                tmp_ref[pl.ds(k * slab, n), :] += g_ref[pl.ds(k * slab + by, n), :]
    rawr_ref[...] = acc
    for k in range(slabs):
        rows = pl.ds(k * slab, slab)
        total = tmp_ref[rows, :].astype(BF16)
        gnode_ref[rows, :] += dot_nt(total, w1s)
        rawr_ref[...] += dot_t(node_ref[rows, :], total)
    raw_ref[h:2 * h, :] = rawr_ref[...]
    for k in range(4):
        raw_ref[7 * h + k:7 * h + k + 1, :] = jnp.sum(bias_ref[k], axis=0, keepdims=True)
    rawb_ref[...] = raw_ref[...].astype(BF16)


MESH = pl.DeviceIdType.MESH
AXES = ("gx", "gy", "gz")


def neighbours():
    here = [lax.axis_index(a) for a in AXES]
    out = []
    for k, a in enumerate(AXES):
        count = lax.axis_size(a)
        for step in (1, count - 1):
            at = list(here)
            at[k] = lax.rem(here[k] + step, count)
            out.append(tuple(at))
    return out


def halo_kernel(dims, node_ref, *refs):
    outs, sends, lands, tmp_ref, send_sem, recv_sem = (
        refs[:6], refs[6:12], refs[12:18], refs[18], refs[19], refs[20]
    )
    sx, sy, sz = dims
    plane = sy * sz
    cells = sx * plane
    ids = neighbours()
    barrier = pltpu.get_barrier_semaphore()
    for who in ids:
        pl.semaphore_signal(barrier, inc=1, device_id=who, device_id_type=MESH)
    for k in range(cells // 256):
        rows = pl.ds(k * 256, 256)
        tmp_ref[rows, :] = node_ref[rows, :].astype(F32)
    sends[4][...] = tmp_ref[pl.ds(sz - 1, sx * sy, stride=sz), :].astype(BF16)
    sends[5][...] = tmp_ref[pl.ds(0, sx * sy, stride=sz), :].astype(BF16)
    sends[0][...] = node_ref[pl.ds(cells - plane, plane), :]
    sends[1][...] = node_ref[pl.ds(0, plane), :]
    sends[2][...] = jnp.concatenate(
        [tmp_ref[pl.ds(i * plane + plane - sz, sz), :] for i in range(sx)], axis=0
    ).astype(BF16)
    sends[3][...] = jnp.concatenate(
        [tmp_ref[pl.ds(i * plane, sz), :] for i in range(sx)], axis=0
    ).astype(BF16)
    pl.semaphore_wait(barrier, 6)
    copies = []
    for d in (4, 5, 0, 1, 2, 3):
        copy = pltpu.make_async_remote_copy(
            src_ref=sends[d], dst_ref=lands[d ^ 1],
            send_sem=send_sem.at[d], recv_sem=recv_sem.at[d ^ 1],
            device_id=ids[d], device_id_type=MESH,
        )
        copy.start()
        copies.append((d, copy))
    for d, copy in copies:
        copy.wait_send()
    for d, copy in copies:
        copy.wait_recv()
        outs[d ^ 1][...] = lands[d ^ 1][...]


def reduce_kernel(dims, raw_ref, gnode_ref, *refs):
    faces = refs[:6]
    gout_ref, allout_ref = refs[6:8]
    part_ref, sum_ref, all_ref, tmp_ref = refs[8:12]
    lands = refs[12:18]
    rs_send, rs_recv, ag_send, ag_recv, halo_send, halo_recv = refs[18:24]
    sx, sy, sz = dims
    plane = sy * sz
    cells = sx * plane
    h = gnode_ref.shape[1]
    nx, ny, nz = [lax.axis_size(a) for a in AXES]
    n = nx * ny * nz
    ix, iy, iz = [lax.axis_index(a) for a in AXES]
    me = (ix * ny + iy) * nz + iz

    def rank(k):
        return lax.rem(me + k, n)

    def device(p):
        return (p // (ny * nz), p // nz % ny, p % nz)

    barrier = pltpu.get_barrier_semaphore()

    @pl.loop(1, n)
    def _(k):
        pl.semaphore_signal(barrier, inc=1, device_id=device(rank(k)), device_id_type=MESH)

    for k in range(cells // 256):
        rows = pl.ds(k * 256, 256)
        tmp_ref[rows, :] = gnode_ref[rows, :]
    pl.semaphore_wait(barrier, n - 1)

    def scatter(k):
        p = rank(k)
        return pltpu.make_async_remote_copy(
            src_ref=raw_ref.at[p], dst_ref=part_ref.at[k],
            send_sem=rs_send.at[k], recv_sem=rs_recv.at[k],
            device_id=device(p), device_id_type=MESH,
        )

    def spread(k):
        p = rank(k)
        return pltpu.make_async_remote_copy(
            src_ref=sum_ref, dst_ref=all_ref.at[me],
            send_sem=ag_send.at[k], recv_sem=ag_recv.at[k],
            device_id=device(p), device_id_type=MESH,
        )

    @pl.loop(1, n)
    def _(k):
        scatter(k).start()

    ids = neighbours()
    halos = []
    for d in range(6):
        halos.append(pltpu.make_async_remote_copy(
            src_ref=faces[d], dst_ref=lands[d],
            send_sem=halo_send.at[d], recv_sem=halo_recv.at[d],
            device_id=ids[d], device_id_type=MESH,
        ))
        halos[-1].start()

    @pl.loop(1, n)
    def _(k):
        scatter(k).wait_recv()

    def add(k, total):
        return total + part_ref[k].astype(F32)

    total = lax.fori_loop(1, n, add, raw_ref[me].astype(F32)).astype(BF16)
    sum_ref[...] = total
    all_ref[me] = total

    @pl.loop(1, n)
    def _(k):
        spread(k).start()

    for d in range(6):
        halos[d].wait_recv()
    tmp_ref[pl.ds(0, plane), :] += lands[0][...].astype(F32)
    tmp_ref[pl.ds(cells - plane, plane), :] += lands[1][...].astype(F32)
    low, high = lands[2][...].astype(F32), lands[3][...].astype(F32)
    for i in range(sx):
        tmp_ref[pl.ds(i * plane, sz), :] += low[i * sz:(i + 1) * sz]
        tmp_ref[pl.ds(i * plane + plane - sz, sz), :] += high[i * sz:(i + 1) * sz]
    tmp_ref[pl.ds(0, sx * sy, stride=sz), :] += lands[4][...].astype(F32)
    tmp_ref[pl.ds(sz - 1, sx * sy, stride=sz), :] += lands[5][...].astype(F32)
    for k in range(cells // 256):
        rows = pl.ds(k * 256, 256)
        gout_ref[rows, :] = tmp_ref[rows, :].astype(BF16)

    @pl.loop(1, n)
    def _(k):
        spread(k).wait_recv()

    allout_ref[...] = all_ref[...]

    @pl.loop(1, n)
    def _(k):
        scatter(k).wait_send()
        spread(k).wait_send()

    for d in range(6):
        halos[d].wait_send()


def finish_kernel(all_ref, gin_ref, gout_ref, w1e_ref, w2e_ref, w1n_ref, w2n_ref, bias_ref):
    h = gin_ref.shape[1]
    gout_ref[...] = gin_ref[...]
    full = all_ref[...].astype(F32).reshape(-1, h)
    squares = jnp.sum(jnp.sum(fold_rows(full * full), axis=0, keepdims=True), axis=1, keepdims=True)
    factor = 1.0 / jnp.maximum(1.0, jnp.sqrt(squares / (7 * h * h + 4 * h)))
    at = 0
    for ref in (w1e_ref, w2e_ref, w1n_ref, w2n_ref, bias_ref):
        rows = ref.shape[0]
        ref[...] = full[at:at + rows] * factor
        at += rows


def on_device(
    node_latent, edge_latent, senders, receivers,
    w1_edge, b1_edge, w2_edge, b2_edge, w1_node, b1_node, w2_node,
    cot_node, cot_edge,
):
    sx, sy, sz, lat = node_latent.shape
    cells = sx * sy * sz
    edges = edge_latent.shape[3]
    own = node_latent.reshape(cells, lat)
    vmem = pl.BlockSpec(memory_space=pltpu.VMEM)
    smem = pl.BlockSpec(memory_space=pltpu.SMEM)
    face_rows = [sy * sz, sy * sz, sx * sz, sx * sz, sx * sy, sx * sy]
    dims = (sx, sy, sz)
    faces = pl.pallas_call(
        functools.partial(halo_kernel, dims),
        out_shape=[jax.ShapeDtypeStruct((n, lat), BF16) for n in face_rows],
        in_specs=[vmem],
        out_specs=[vmem] * 6,
        scratch_shapes=[pltpu.VMEM((n, lat), BF16) for n in face_rows] * 2
        + [
            pltpu.VMEM((cells, lat), F32),
            pltpu.SemaphoreType.DMA((6,)),
            pltpu.SemaphoreType.DMA((6,)),
        ],
        compiler_params=pltpu.CompilerParams(collective_id=0, has_side_effects=True),
    )(own)
    r = receivers.reshape(edges)
    s = senders.reshape(edges)
    padded = ((r // (sy * sz) + 1) * (sy + 2) + r // sz % sy + 1) * (sz + 2) + r % sz + 1
    diff = s - padded
    step_x = (sy + 2) * (sz + 2)
    step_y = sz + 2
    direction = jnp.where(
        diff == step_x, 0,
        jnp.where(
            diff == -step_x, 1,
            jnp.where(
                diff == step_y, 2, jnp.where(diff == -step_y, 3, jnp.where(diff == 1, 4, 5))
            ),
        ),
    )
    stride = 1
    while stride < cells + WIDE:
        stride *= 2
    tiles = edges // TILE
    keys = (direction * stride + r).reshape(tiles, TILE)
    grouped = r.reshape(tiles, TILE)
    base = grouped[:, 0] // ROUND * ROUND
    counts = (grouped[:, -1] - base) // WIN + 1

    devices = 1
    for axis in AXES:
        devices *= lax.axis_size(axis)
    chunk = -(-(7 * lat + 4) // (16 * devices)) * 16
    outs = pl.pallas_call(
        functools.partial(layer_kernel, dims, stride),
        out_shape=[
            jax.ShapeDtypeStruct((cells, lat), F32),
            jax.ShapeDtypeStruct((edges, lat), BF16),
            jax.ShapeDtypeStruct((devices * chunk, lat), BF16),
        ] + [jax.ShapeDtypeStruct((n, lat), BF16) for n in face_rows],
        in_specs=[smem] * 2 + [vmem] * 18,
        out_specs=[vmem] * 9,
        scratch_shapes=[
            pltpu.VMEM((6, cells + WIDE, lat), BF16),
            pltpu.VMEM((cells, lat), F32),
            pltpu.VMEM((cells, lat), F32),
            pltpu.VMEM((cells, lat), F32),
            pltpu.VMEM((edges, lat), F32),
            pltpu.VMEM((cells + WIDE, lat), F32),
            pltpu.VMEM((cells + WIDE, lat), BF16),
            pltpu.VMEM((4, 8, lat), F32),
            pltpu.VMEM((lat, lat), F32),
            pltpu.VMEM((devices * chunk, lat), F32),
        ] + [pltpu.VMEM((cells + WIDE, lat), F32)] * 6,
        compiler_params=pltpu.CompilerParams(vmem_limit_bytes=60 * 1024 * 1024),
        cost_estimate=pl.CostEstimate(
            flops=40 * edges * lat * lat, bytes_accessed=6 * edges * lat, transcendentals=0
        ),
    )(
        base, counts,
        own, edge_latent.reshape(edges, lat), cot_edge.reshape(edges, lat),
        cot_node.reshape(cells, lat), keys,
        w1_edge, b1_edge.reshape(1, lat), w2_edge, b2_edge.reshape(1, lat),
        w1_node, b1_node.reshape(1, lat), w2_node,
        *faces,
    )
    gnode, gedge, raw = outs[:3]
    gsum, full = pl.pallas_call(
        functools.partial(reduce_kernel, dims),
        out_shape=[
            jax.ShapeDtypeStruct((cells, lat), BF16),
            jax.ShapeDtypeStruct((devices, chunk, lat), BF16),
        ],
        in_specs=[vmem] * 8,
        out_specs=[vmem] * 2,
        scratch_shapes=[
            pltpu.VMEM((devices, chunk, lat), BF16),
            pltpu.VMEM((chunk, lat), BF16),
            pltpu.VMEM((devices, chunk, lat), BF16),
            pltpu.VMEM((cells, lat), F32),
        ]
        + [pltpu.VMEM((n, lat), BF16) for n in face_rows]
        + [pltpu.SemaphoreType.DMA((devices,))] * 4
        + [pltpu.SemaphoreType.DMA((6,))] * 2,
        compiler_params=pltpu.CompilerParams(collective_id=1, has_side_effects=True),
    )(raw.reshape(devices, chunk, lat), gnode, *outs[3:])
    out = pl.pallas_call(
        finish_kernel,
        out_shape=[
            jax.ShapeDtypeStruct((cells, lat), BF16),
            jax.ShapeDtypeStruct((3 * lat, lat), F32),
            jax.ShapeDtypeStruct((lat, lat), F32),
            jax.ShapeDtypeStruct((2 * lat, lat), F32),
            jax.ShapeDtypeStruct((lat, lat), F32),
            jax.ShapeDtypeStruct((4, lat), F32),
        ],
        in_specs=[vmem] * 2,
        out_specs=[vmem] * 6,
    )(full, gsum)
    return (
        out[0].reshape(node_latent.shape),
        gedge.reshape(edge_latent.shape),
        *out[1:],
    )


def solution(mesh):
    cell = P("gx", "gy", "gz", None)
    edge = P("gx", "gy", "gz", None, None)
    return jax.shard_map(
        on_device,
        mesh=mesh,
        in_specs=(cell, edge, cell, cell, P(), P(), P(), P(), P(), P(), P(), cell, edge),
        out_specs=(cell, edge, P(), P(), P(), P(), P()),
        check_vma=False,
    )
```
